128 devices in a mesh: gx: 16 (over y, z), gy: 8 (over x, core).
Axes of the slice: x: 4, y: 4, z: 4, core: 2. Of those that a mesh axis runs over, the one named last changes fastest.
Arguments:
- table: float32 [4, 131072, 128], P(None, 'gx'), may hold values from -2.1 to 2.1
- lookup_owner: int32 [4, 32768, 16, 1], P(None, ('gx', 'gy')), may hold values from 0 to 15; in each aligned block of 4096 rows (0 to 4095, 4096 to 8191, ..., all dimensions but the last counted through in order) at most 512 rows name the same one
- lookup_row: int32 [4, 32768, 16], P(None, ('gx', 'gy')), may hold values from 0 to 8191
- bag_length: int32 [4, 32768], P(None, ('gx', 'gy')), may hold values from 1 to 16
- top_in: bfloat16 [512, 8192], P(None, 'gy'), may hold values from -0.25 to 0.25
- top_bias: float32 [8192], P('gy'), may hold values from -3 to 3
- top_out: bfloat16 [8192, 1024], P('gy'), may hold values from -0.0625 to 0.0625
Outputs:
- scored: bfloat16 [32768, 1024], P(('gx', 'gy'))
The draws below stay inside these ranges and needn't reach their ends.
Inputs may be any that keep to these rules, and one draw needn't show every extreme that they name: `lookup_owner`: in every aligned block of 4096 entries (the lookups of one table from the samples of one device) no owner is named more than 512 times; some blocks reach 512.
All inputs are finite; a program needn't handle non-finite values.
Results may differ from the reference program's by a relative error of at most 0.0057.
Values may be sent and summed in bfloat16 or wider, within the bound.
No kernel may reach another device: no remote copies, remote signals or barrier semaphores. Data moves between devices by JAX's collectives and lax.ppermute only.
A program may use at most 128 MiB of HBM per device.

```python
import math
import jax
import jax.numpy as jnp
import numpy as np
from jax import lax

EMB = 128
TABLES = 4
ROWS_DEV = 8192
SAMPLES_DEV = 256
BAG = 16
TOP_W = 8192
OUT_W = 1024
ROWS = 131072
BATCH = 32768
CAP = 512
N_GX = 16


def set_ends(values, key, smallest, high):
    longest = values.shape.index(max(values.shape))
    spots = []
    for shift in (0, 1):
        where = [jax.random.randint(jax.random.fold_in(key, axis), (), 0, length) for axis, length in enumerate(values.shape)]
        where[longest] = (where[longest] + shift) % values.shape[longest]
        spots.append(tuple(where))
    return values.at[spots[0]].set(smallest).at[spots[1]].set(high)


def levels(stream_key, extent, cuts, low, top_value):
    level, own = 1.0, jax.random.fold_in(stream_key, 6)
    for dim, blocks in cuts:
        steps = jnp.exp(jax.random.uniform(jax.random.fold_in(own, dim), (blocks,), jnp.float32, low / len(cuts), top_value / len(cuts)))
        level = level * jnp.repeat(steps, extent[dim] // blocks).reshape([-1 if axis == dim else 1 for axis in range(len(extent))])
    return level


def rank_bounds(number_of, lean):
    portions = [(1 << 20) // math.isqrt(rank ** lean) + 1 for rank in range(1, number_of + 1)]
    width = 1 + sum(portions) // (1 << 30)
    return np.cumsum(np.array([max(1, weight // width) for weight in portions]))


def ranked_ids(stream_key, extent, number_of, skew):
    table = rank_bounds(number_of, skew)
    pick = jax.random.randint(jax.random.fold_in(stream_key, 1), extent, 0, int(table[number_of - 1]))
    rank = jnp.searchsorted(jnp.asarray(table, jnp.int32), pick, side="right")
    return jax.random.permutation(jax.random.fold_in(stream_key, 2), number_of)[rank].astype(jnp.int32)


def deal_out(stream_key, own, number, rows, number_of, top, most, slope):
    sequence = jax.random.permutation(stream_key, number_of)
    crowded, common = portions_of(number_of, rows * top, most, slope, True), portions_of(number_of, rows * top, most, slope, False)
    places = jnp.arange(number_of)

    def named(tallies, turn):
        used = int((tallies > 0).sum())
        fixed = max(1, used // 4)
        passed = fixed + (places - fixed + turn * (used - fixed)) % max(1, number_of - fixed)
        return jnp.zeros((number_of,), jnp.int32).at[sequence[jnp.where(places < fixed, places, passed)]].set(jnp.asarray(tallies, jnp.int32))

    tallies = jnp.where(number % 4 == 0, named(crowded, number // 4), named(common, number - number // 4 - 1))
    mixed = jax.random.permutation(jax.random.fold_in(own, 3), number_of)
    donor, receiver = mixed[0:number_of // 2 * 2:2], mixed[1:number_of // 2 * 2:2]
    margin = jnp.minimum(tallies[donor] - 1, most - tallies[receiver]) // 2
    margin = jnp.where((donor == sequence[0]) | (receiver == sequence[0]) | (tallies[receiver] == 0), 0, jnp.maximum(margin, 0))
    passed = jax.random.randint(jax.random.fold_in(own, 4), (number_of // 2,), 0, 1 << 20) % (margin + 1)
    tallies = tallies.at[donor].add(-passed).at[receiver].add(passed)
    labels = jnp.searchsorted(jnp.cumsum(tallies), jnp.arange(rows * top), side="right").astype(jnp.int32)
    table = labels.reshape(top, rows).T
    table = table[jax.random.permutation(jax.random.fold_in(own, 1), rows)]
    turn = jax.random.randint(jax.random.fold_in(own, 2), (rows, 1), 0, top)
    return jnp.take_along_axis(table, (jnp.arange(top)[None, :] + turn) % top, axis=1)


def portions_of(amount, total, reach, skew, full):
    weights = [(1 << 20) // math.isqrt(rank ** skew) + 1 for rank in range(1, amount + 1)]
    largest = reach if full else min(reach, max(-(-total // amount), total * weights[0] // sum(weights)))
    least = 1 if total - largest >= amount - 1 else 0
    counts, rest = [largest] + [least] * (amount - 1), total - largest - least * (amount - 1)
    while rest > 0:
        free = [i for i in range(1, amount) if counts[i] < largest] or [i for i in range(1, amount) if counts[i] < reach]
        pool, budget = sum([weights[i] for i in free]), rest
        for i in free:
            extra = min(reach - counts[i], max(1, budget * weights[i] // pool), rest)
            counts[i] = counts[i] + extra
            rest = rest - extra
    return np.array(counts)


def noise(rng, shape, deviation, bound, split=(), kind=jnp.bfloat16):
    drawn = jax.random.normal(rng, shape, jnp.float32) * deviation
    if len(split) > 0:
        drawn = levels(rng, shape, split, -0.22, 0.18) * drawn
    return jnp.clip(drawn, min=-bound, max=bound).astype(kind)


def setup_inputs(seed: int = 0) -> dict:
    seeds = jax.random.split(jax.random.key(seed), 8)
    table = noise(seeds[0], (TABLES, ROWS, EMB), 0.35, 2.1, ((1, 16),), jnp.float32)
    lookup_owner_keys = jax.random.split(jax.random.fold_in(seeds[1], 1), TABLES * BATCH * BAG // (SAMPLES_DEV * BAG))
    lookup_owner_turns = jax.random.permutation(jax.random.fold_in(seeds[1], 3), TABLES * BATCH * BAG // (SAMPLES_DEV * BAG))
    lookup_owner = jax.vmap(lambda own, number: deal_out(jax.random.fold_in(seeds[1], 2), own, number, SAMPLES_DEV * BAG, N_GX, 1, CAP, 1))(lookup_owner_keys, lookup_owner_turns).reshape((TABLES, BATCH, BAG, 1))
    lookup_row = set_ends(ranked_ids(seeds[2], (TABLES, BATCH, BAG), ROWS_DEV, 2), jax.random.fold_in(seeds[2], 3), 0, ROWS_DEV - 1).astype(jnp.int32)
    bag_length = set_ends(jax.random.randint(seeds[3], (TABLES, BATCH), 1, BAG + 1), jax.random.fold_in(seeds[3], 1), 1, BAG).astype(jnp.int32)
    top_in = noise(seeds[4], (TABLES * EMB, TOP_W), (TABLES * EMB) ** -0.5, 0.25, ((1, 8),))
    top_bias = noise(seeds[5], (TOP_W,), 0.5, 3.0, ((0, 8),), jnp.float32)
    top_out = noise(seeds[6], (TOP_W, OUT_W), TOP_W ** -0.5, 0.0625, ((0, 8),))
    return dict(table=table, lookup_owner=lookup_owner, lookup_row=lookup_row, bag_length=bag_length, top_in=top_in, top_bias=top_bias, top_out=top_out)


def pool_table(pieces):
    table_part, index_part, live_part = pieces
    fetched = jnp.take(table_part, index_part, axis=0)
    return jnp.sum(jnp.where(live_part[..., None], fetched, jnp.float32(0.0)), axis=1)


def reference(table, lookup_owner, lookup_row, bag_length, top_in, top_bias, top_out):
    row_index = (lookup_owner[..., 0] * ROWS_DEV + lookup_row).astype(jnp.int32)
    is_live = jnp.arange(BAG, dtype=jnp.int32)[None, None, :] < bag_length[:, :, None]
    pooled = lax.map(pool_table, (table, row_index, is_live))
    features = jnp.transpose(pooled, (1, 0, 2)).reshape(BATCH, TABLES * EMB).astype(jnp.bfloat16)
    blocks = features.reshape(N_GX, BATCH // N_GX, TABLES * EMB)

    def one_block(block):
        pre_act = jnp.dot(block, top_in, preferred_element_type=jnp.float32) + top_bias
        hidden_rows = jnp.maximum(pre_act, 0.0).astype(jnp.bfloat16)
        return jnp.dot(hidden_rows, top_out, preferred_element_type=jnp.float32).astype(jnp.bfloat16)

    scored = lax.map(one_block, blocks)
    return scored.reshape(BATCH, OUT_W)
```

```python
import functools

import jax
import jax.numpy as jnp
from jax import lax
from jax.experimental import pallas as pl
from jax.experimental.pallas import tpu as pltpu
from jax.sharding import PartitionSpec as P


TABLES = 4
SAMPLES = 256
BAG = 16
OWNERS = 16
CAP = 512
ROWS_DEV = 8192
EMB = 128
UNROLL = 16
STEP = 4
VALID = 1 << 13
BAG_SHIFT = 14


def iota(shape, dim):
    return lax.broadcasted_iota(jnp.int32, shape, dim)


def ones_where(mask):
    return jnp.where(mask, 1.0, 0.0).astype(jnp.bfloat16)


def dispatch_kernel(own_ref, row_ref, out_ref):
    before = ones_where(iota((256, 256), 0) < iota((256, 256), 1))
    r, c = iota((256, 256), 0), iota((256, 256), 1)
    earlier = ones_where(((r & 15) == (c & 15)) & ((c >> 4) < (r >> 4)))
    ones = jnp.ones((256, 256), jnp.bfloat16)
    same = ones_where(iota((16, 256), 0) == (iota((16, 256), 1) & 15))
    owner_iota = iota((16, 16, 256), 1)
    for t in range(TABLES):
        own = own_ref[t]
        mark = (own[:, None, :] == owner_iota).reshape(256, 256)
        onehot = ones_where(mark)
        rank = jnp.dot(onehot, before, preferred_element_type=jnp.float32)
        lead = jnp.dot(earlier, onehot, preferred_element_type=jnp.float32)
        rank += jnp.dot(lead.astype(jnp.bfloat16), ones, preferred_element_type=jnp.float32)
        rank = jnp.sum(jnp.where(mark, rank, 0.0).reshape(16, 16, 256), axis=1).astype(jnp.int32)
        total = jnp.dot(same, onehot, preferred_element_type=jnp.float32)
        total = jnp.dot(total.astype(jnp.bfloat16), ones, preferred_element_type=jnp.float32)
        out_ref[:, 16 + t, :] = total[:, :128].astype(jnp.int32)
        hi = own * 4 + (rank >> 7)
        lo = rank & 127
        row = row_ref[t]
        low = (row & 255).astype(jnp.float32)
        high = ((row >> 8) + (VALID >> 8)).astype(jnp.float32)
        bag = iota((1, 256), 1).astype(jnp.float32)
        acc = jnp.zeros((192, 128), jnp.float32)
        for s in range(BAG):
            left = hi[s : s + 1, :] == iota((64, 256), 0)
            planes = jnp.concatenate(
                [
                    jnp.where(left, low[s : s + 1, :], 0.0),
                    jnp.where(left, high[s : s + 1, :], 0.0),
                    jnp.where(left, bag, 0.0),
                ],
                axis=0,
            ).astype(jnp.bfloat16)
            right = ones_where(lo[s : s + 1, :] == iota((128, 256), 0))
            acc += lax.dot_general(
                planes, right, (((1,), (1,)), ((), ())), preferred_element_type=jnp.float32
            )
        acc = acc.astype(jnp.int32)
        code = acc[:64] | (acc[64:128] << 8) | (acc[128:] << BAG_SHIFT)
        out_ref[:, 4 * t : 4 * t + 4, :] = code.reshape(OWNERS, 4, 128)
    out_ref[:, 20:, :] = jnp.zeros((OWNERS, 4, 128), jnp.int32)


def pool_kernel(rows_ref, count_ref, bags_ref, table_ref, out_ref, buf_ref):
    step = pl.program_id(0)

    @pl.when(step == 0)
    def _():
        buf_ref[...] = jnp.zeros_like(buf_ref)

    for q in range(STEP):
        source = step * STEP + q
        start = pl.multiple_of(source * CAP, CAP)

        def fetch(group, carry, start=start, q=q):
            base = pl.multiple_of(group * UNROLL, UNROLL)
            for k in range(UNROLL):
                row = rows_ref[start + base + k]
                buf_ref[q, pl.ds(base + k, 1), :] = table_ref[pl.ds(row, 1), :]
            return carry

        lax.fori_loop(0, (count_ref[source] + UNROLL - 1) // UNROLL, fetch, 0)
    for q in range(STEP):
        pick = ones_where(bags_ref[q : q + 1, :] == iota((SAMPLES, CAP), 0))
        out_ref[q] = jnp.dot(
            pick, buf_ref[q].astype(jnp.bfloat16), preferred_element_type=jnp.float32
        ).astype(out_ref.dtype)


def pool_table(t, rows, counts, bags, table):
    return pl.pallas_call(
        pool_kernel,
        grid_spec=pltpu.PrefetchScalarGridSpec(
            num_scalar_prefetch=2,
            grid=(OWNERS // STEP,),
            in_specs=[
                pl.BlockSpec((None, STEP, CAP), lambda i, *_: (i, 0, 0)),
                pl.BlockSpec((None, ROWS_DEV, EMB), lambda i, *_: (t, 0, 0)),
            ],
            out_specs=pl.BlockSpec((STEP, SAMPLES, EMB), lambda i, *_: (i, 0, 0)),
            scratch_shapes=[pltpu.VMEM((STEP, CAP, EMB), jnp.float32)],
        ),
        out_shape=jax.ShapeDtypeStruct((OWNERS, SAMPLES, EMB), jnp.bfloat16),
        compiler_params=pltpu.CompilerParams(vmem_limit_bytes=24 << 20),
        cost_estimate=pl.CostEstimate(
            flops=20_000_000_000, transcendentals=0, bytes_accessed=6_000_000
        ),
        name=f"pool_{t}",
    )(rows, counts, bags.reshape(OWNERS // STEP, STEP, CAP), table)


def along_x(array, shift):
    return lax.ppermute(
        array, "gy", [(x * 2 + c, ((x + shift) % 4) * 2 + c) for x in range(4) for c in range(2)]
    )


def partner(array):
    return lax.ppermute(array, "gy", [(k, k ^ 1) for k in range(8)])


def local(table, lookup_owner, lookup_row, bag_length, top_in, top_bias, top_out):
    w_in = (top_in, partner(top_in))
    w_out = (top_out, partner(top_out))
    bias = (top_bias, partner(top_bias))

    owner = jnp.transpose(lookup_owner[..., 0], (0, 2, 1))
    live = jnp.arange(BAG, dtype=jnp.int32)[None, :, None] < bag_length[:, None, :]
    owner = jnp.where(live, owner, OWNERS)
    row = jnp.transpose(lookup_row, (0, 2, 1))
    codes = pl.pallas_call(
        dispatch_kernel,
        out_shape=jax.ShapeDtypeStruct((OWNERS, 24, 128), jnp.int32),
        name="dispatch",
    )(owner, row)
    codes = lax.all_to_all(codes, "gx", 0, 0, tiled=True)
    counts = codes[:, 16:20, 0].T
    codes = jnp.transpose(codes[:, :16, :].reshape(OWNERS, TABLES, CAP), (1, 0, 2))
    rows = (codes & (ROWS_DEV - 1)).reshape(TABLES, OWNERS * CAP)
    bags = jnp.where((codes & VALID) != 0, codes >> BAG_SHIFT, SAMPLES)

    features = []
    for t in range(TABLES):
        part = pool_table(t, rows[t], counts[t], bags[t], table)
        part = lax.all_to_all(part, "gx", 0, 0, tiled=True)
        features.append(jnp.sum(part.astype(jnp.float32), axis=0).astype(jnp.bfloat16))
    halves = [jnp.concatenate(features[:2], axis=1), jnp.concatenate(features[2:], axis=1)]
    outs = {}
    for shift in (2, 1, 3, 0):
        moved = [along_x(h, shift) if shift else h for h in halves]
        block = jnp.concatenate(moved, axis=1)
        total = 0.0
        for k in range(2):
            pre = jnp.dot(block, w_in[k], preferred_element_type=jnp.float32) + bias[k]
            hidden = jnp.maximum(pre, 0.0).astype(jnp.bfloat16)
            total += jnp.dot(hidden, w_out[k], preferred_element_type=jnp.float32)
        outs[shift] = along_x(total.astype(jnp.bfloat16), -shift) if shift else total
    scored = outs[0]
    for shift in (1, 2, 3):
        scored += outs[shift].astype(jnp.float32)
    return scored.astype(jnp.bfloat16)


def solution(mesh):
    return jax.shard_map(
        local,
        mesh=mesh,
        in_specs=(
            P(None, "gx", None),
            P(None, ("gx", "gy"), None, None),
            P(None, ("gx", "gy"), None),
            P(None, ("gx", "gy")),
            P(None, "gy"),
            P("gy"),
            P("gy", None),
        ),
        out_specs=P(("gx", "gy"), None),
        check_vma=False,
    )
```

```python
import functools

import jax
import jax.numpy as jnp
from jax import lax
from jax.experimental import pallas as pl
from jax.experimental.pallas import tpu as pltpu
from jax.sharding import PartitionSpec as P


TABLES = 4
SAMPLES = 256
BAG = 16
OWNERS = 16
CAP = 512
ROWS_DEV = 8192
EMB = 128
UNROLL = 16
STEP = 4
VALID = 1 << 13
BAG_SHIFT = 14
CHUNKS = (2, 2)


def iota(shape, dim):
    return lax.broadcasted_iota(jnp.int32, shape, dim)


def ones_where(mask):
    return jnp.where(mask, 1.0, 0.0).astype(jnp.bfloat16)


def dispatch_kernel(own_ref, row_ref, out_ref):
    before = ones_where(iota((256, 256), 0) < iota((256, 256), 1))
    r, c = iota((256, 256), 0), iota((256, 256), 1)
    earlier = ones_where(((r & 15) == (c & 15)) & ((c >> 4) < (r >> 4)))
    ones = jnp.ones((256, 256), jnp.bfloat16)
    same = ones_where(iota((16, 256), 0) == (iota((16, 256), 1) & 15))
    owner_iota = iota((16, 16, 256), 1)
    for t in range(TABLES):
        own = own_ref[t]
        mark = (own[:, None, :] == owner_iota).reshape(256, 256)
        onehot = ones_where(mark)
        rank = jnp.dot(onehot, before, preferred_element_type=jnp.float32)
        lead = jnp.dot(earlier, onehot, preferred_element_type=jnp.float32)
        rank += jnp.dot(lead.astype(jnp.bfloat16), ones, preferred_element_type=jnp.float32)
        rank = jnp.sum(jnp.where(mark, rank, 0.0).reshape(16, 16, 256), axis=1).astype(jnp.int32)
        total = jnp.dot(same, onehot, preferred_element_type=jnp.float32)
        total = jnp.dot(total.astype(jnp.bfloat16), ones, preferred_element_type=jnp.float32)
        out_ref[:, 16 + t, :] = total[:, :128].astype(jnp.int32)
        hi = own * 4 + (rank >> 7)
        lo = rank & 127
        row = row_ref[t]
        low = (row & 255).astype(jnp.float32)
        high = ((row >> 8) + (VALID >> 8)).astype(jnp.float32)
        bag = iota((1, 256), 1).astype(jnp.float32)
        acc = jnp.zeros((192, 128), jnp.float32)
        for s in range(BAG):
            left = hi[s : s + 1, :] == iota((64, 256), 0)
            planes = jnp.concatenate(
                [
                    jnp.where(left, low[s : s + 1, :], 0.0),
                    jnp.where(left, high[s : s + 1, :], 0.0),
                    jnp.where(left, bag, 0.0),
                ],
                axis=0,
            ).astype(jnp.bfloat16)
            right = ones_where(lo[s : s + 1, :] == iota((128, 256), 0))
            acc += lax.dot_general(
                planes, right, (((1,), (1,)), ((), ())), preferred_element_type=jnp.float32
            )
        acc = acc.astype(jnp.int32)
        code = acc[:64] | (acc[64:128] << 8) | (acc[128:] << BAG_SHIFT)
        out_ref[:, 4 * t : 4 * t + 4, :] = code.reshape(OWNERS, 4, 128)
    out_ref[:, 20:, :] = jnp.zeros((OWNERS, 4, 128), jnp.int32)


def pool_kernel(first, rows_ref, count_ref, bags_ref, table_ref, out_ref, buf_ref, held_ref, sem):
    tables = held_ref.shape[0]
    turn, step = pl.program_id(0), pl.program_id(1)

    def load(t):
        return pltpu.make_async_copy(table_ref.at[first + t], held_ref.at[t], sem.at[t])

    @pl.when((turn == 0) & (step == 0))
    def _():
        for t in range(tables):
            load(t).start()
        buf_ref[...] = jnp.zeros_like(buf_ref)

    for t in range(tables):

        @pl.when((turn == t) & (step == 0))
        def _(t=t):
            load(t).wait()

    for q in range(STEP):
        source = (turn * (OWNERS // STEP) + step) * STEP + q
        start = pl.multiple_of(source * CAP, CAP)

        def fetch(group, carry, start=start, q=q):
            base = pl.multiple_of(group * UNROLL, UNROLL)
            for k in range(UNROLL):
                row = rows_ref[start + base + k]
                buf_ref[q, pl.ds(base + k, 1), :] = held_ref[turn, pl.ds(row, 1), :]
            return carry

        lax.fori_loop(0, (count_ref[source] + UNROLL - 1) // UNROLL, fetch, 0)
    for q in range(STEP):
        pick = ones_where(bags_ref[q : q + 1, :] == iota((SAMPLES, CAP), 0))
        out_ref[q] = jnp.dot(
            pick, buf_ref[q].astype(jnp.bfloat16), preferred_element_type=jnp.float32
        ).astype(out_ref.dtype)


def pool_tables(first, tables, rows, counts, bags, table):
    steps = OWNERS // STEP
    return pl.pallas_call(
        functools.partial(pool_kernel, first),
        grid_spec=pltpu.PrefetchScalarGridSpec(
            num_scalar_prefetch=2,
            grid=(tables, steps),
            in_specs=[
                pl.BlockSpec((None, STEP, CAP), lambda t, i, *_: (t * steps + i, 0, 0)),
                pl.BlockSpec(memory_space=pltpu.HBM),
            ],
            out_specs=pl.BlockSpec((STEP, SAMPLES, EMB), lambda t, i, *_: (i, 0, t)),
            scratch_shapes=[
                pltpu.VMEM((STEP, CAP, EMB), jnp.float32),
                pltpu.VMEM((tables, ROWS_DEV, EMB), jnp.float32),
                pltpu.SemaphoreType.DMA((tables,)),
            ],
        ),
        out_shape=jax.ShapeDtypeStruct((OWNERS, SAMPLES, tables * EMB), jnp.bfloat16),
        compiler_params=pltpu.CompilerParams(vmem_limit_bytes=54 << 20),
        cost_estimate=pl.CostEstimate(
            flops=10_000_000_000 * tables, transcendentals=0, bytes_accessed=6_000_000
        ),
    )(rows.reshape(-1), counts.reshape(-1), bags.reshape(tables * steps, STEP, CAP), table)


def score_kernel(pieces, chunks, *refs):
    features = refs[:chunks]
    biases = refs[chunks : chunks + pieces]
    w_in = refs[chunks + pieces : chunks + 2 * pieces]
    w_out = refs[chunks + 2 * pieces : chunks + 3 * pieces]
    out_ref, in_buf, out_buf, in_sem, out_sem = refs[chunks + 3 * pieces :]
    copies = []
    for p in range(pieces):
        first = pltpu.make_async_copy(w_in[p], in_buf.at[p], in_sem.at[p])
        second = pltpu.make_async_copy(w_out[p], out_buf.at[p], out_sem.at[p])
        first.start()
        second.start()
        copies.append((first, second))
    total = None
    for p in range(pieces):
        copies[p][0].wait()
        pre = biases[p][...]
        base = 0
        for feature in features:
            width = feature.shape[1]
            pre = pre + jnp.dot(
                feature[...],
                in_buf[p, base : base + width, :],
                preferred_element_type=jnp.float32,
            )
            base += width
        hidden = jnp.maximum(pre, 0.0).astype(jnp.bfloat16)
        copies[p][1].wait()
        part = jnp.dot(hidden, out_buf[p], preferred_element_type=jnp.float32)
        total = part if total is None else total + part
    out_ref[...] = total.astype(out_ref.dtype)


def score(features, biases, w_in, w_out, dtype):
    pieces, chunks = len(w_in), len(features)
    vmem = pl.BlockSpec(memory_space=pltpu.VMEM)
    hbm = pl.BlockSpec(memory_space=pltpu.HBM)
    return pl.pallas_call(
        functools.partial(score_kernel, pieces, chunks),
        in_specs=[vmem] * (chunks + pieces) + [hbm] * (2 * pieces),
        out_specs=vmem,
        scratch_shapes=[
            pltpu.VMEM((pieces, *w_in[0].shape), jnp.bfloat16),
            pltpu.VMEM((pieces, *w_out[0].shape), jnp.bfloat16),
            pltpu.SemaphoreType.DMA((pieces,)),
            pltpu.SemaphoreType.DMA((pieces,)),
        ],
        out_shape=jax.ShapeDtypeStruct((SAMPLES, w_out[0].shape[1]), dtype),
        compiler_params=pltpu.CompilerParams(vmem_limit_bytes=40 << 20),
        cost_estimate=pl.CostEstimate(
            flops=10_000_000_000, transcendentals=0, bytes_accessed=14_000_000
        ),
    )(*features, *biases, *w_in, *w_out)


def to_chip(array, target):
    return lax.ppermute(
        array, "gy", [(x * 2 + c, target(x) * 2 + c) for x in range(4) for c in range(2)]
    )


def to_core(array):
    return lax.ppermute(array, "gy", [(k, k ^ 1) for k in range(8)])


def local(table, lookup_owner, lookup_row, bag_length, top_in, top_bias, top_out):
    own = (top_in, top_bias.reshape(1, -1), top_out)
    far = []
    for array in own:
        far.append(to_chip(array, lambda x: 3 - x))
    near = [to_core(array) for array in own]
    far_near = [to_core(array) for array in far]
    w_in, biases, w_out = zip(own, near, far, far_near)

    owner = jnp.transpose(lookup_owner[..., 0], (0, 2, 1))
    live = jnp.arange(BAG, dtype=jnp.int32)[None, :, None] < bag_length[:, None, :]
    owner = jnp.where(live, owner, OWNERS)
    row = jnp.transpose(lookup_row, (0, 2, 1))
    codes = pl.pallas_call(
        dispatch_kernel,
        out_shape=jax.ShapeDtypeStruct((OWNERS, 24, 128), jnp.int32),
        name="dispatch",
    )(owner, row)
    codes = lax.all_to_all(codes, "gx", 0, 0, tiled=True)
    counts = codes[:, 16:20, 0].T
    codes = jnp.transpose(codes[:, :16, :].reshape(OWNERS, TABLES, CAP), (1, 0, 2))
    rows = (codes & (ROWS_DEV - 1)).reshape(TABLES, OWNERS * CAP)
    bags = jnp.where((codes & VALID) != 0, codes >> BAG_SHIFT, SAMPLES)

    mine, theirs = [], []
    first = 0
    for number in CHUNKS:
        part = slice(first, first + number)
        share = pool_tables(first, number, rows[part], counts[part], bags[part], table)
        first += number
        share = lax.all_to_all(share, "gx", 0, 0, tiled=True)
        chunk = jnp.sum(share.astype(jnp.float32), axis=0).astype(jnp.bfloat16)
        mine.append(chunk)
        theirs.append(to_chip(chunk, lambda x: x ^ 1))
    kept = score(mine, biases, w_in, w_out, jnp.float32)
    sent = score(theirs, biases, w_in, w_out, jnp.bfloat16)
    received = to_chip(sent, lambda x: x ^ 1)
    return (kept + received.astype(jnp.float32)).astype(jnp.bfloat16)


def solution(mesh):
    return jax.shard_map(
        local,
        mesh=mesh,
        in_specs=(
            P(None, "gx", None),
            P(None, ("gx", "gy"), None, None),
            P(None, ("gx", "gy"), None),
            P(None, ("gx", "gy")),
            P(None, "gy"),
            P("gy"),
            P("gy", None),
        ),
        out_specs=P(("gx", "gy"), None),
        check_vma=False,
    )
```

```python
import functools

import jax
import jax.numpy as jnp
from jax import lax
from jax.experimental import pallas as pl
from jax.experimental.pallas import tpu as pltpu
from jax.sharding import PartitionSpec as P


TABLES = 4
SAMPLES = 256
BAG = 16
OWNERS = 16
CAP = 512
ROWS_DEV = 8192
EMB = 128
BLOCK = 64
PIECES = 4
STEP = 8
BAG_SHIFT = 13
CHUNKS = (2, 2)


def iota(shape, dim):
    return lax.broadcasted_iota(jnp.int32, shape, dim)


def ones_where(mask):
    return jnp.where(mask, 1.0, 0.0).astype(jnp.bfloat16)


def dispatch_kernel(own_ref, row_ref, out_ref):
    before = ones_where(iota((256, 256), 0) < iota((256, 256), 1))
    r, c = iota((256, 256), 0), iota((256, 256), 1)
    earlier = ones_where(((r & 15) == (c & 15)) & ((c >> 4) < (r >> 4)))
    ones = jnp.ones((256, 256), jnp.bfloat16)
    same = ones_where(iota((16, 256), 0) == (iota((16, 256), 1) & 15))
    owner_iota = iota((16, 16, 256), 1)
    for t in range(TABLES):
        own = own_ref[t]
        mark = (own[:, None, :] == owner_iota).reshape(256, 256)
        onehot = ones_where(mark)
        rank = jnp.dot(onehot, before, preferred_element_type=jnp.float32)
        lead = jnp.dot(earlier, onehot, preferred_element_type=jnp.float32)
        rank += jnp.dot(lead.astype(jnp.bfloat16), ones, preferred_element_type=jnp.float32)
        rank = jnp.sum(jnp.where(mark, rank, 0.0).reshape(16, 16, 256), axis=1).astype(jnp.int32)
        total = jnp.dot(same, onehot, preferred_element_type=jnp.float32)
        total = jnp.dot(total.astype(jnp.bfloat16), ones, preferred_element_type=jnp.float32)
        out_ref[:, 16 + t, :] = total[:, :128].astype(jnp.int32)
        hi = own * 4 + (rank >> 7)
        lo = rank & 127
        row = row_ref[t]
        low = (row & 255).astype(jnp.float32)
        high = (row >> 8).astype(jnp.float32)
        bag = (iota((1, 256), 1) + 1).astype(jnp.float32)
        acc = jnp.zeros((192, 128), jnp.float32)
        for s in range(BAG):
            left = hi[s : s + 1, :] == iota((64, 256), 0)
            planes = jnp.concatenate(
                [
                    jnp.where(left, low[s : s + 1, :], 0.0),
                    jnp.where(left, high[s : s + 1, :], 0.0),
                    jnp.where(left, bag, 0.0),
                ],
                axis=0,
            ).astype(jnp.bfloat16)
            right = ones_where(lo[s : s + 1, :] == iota((128, 256), 0))
            acc += lax.dot_general(
                planes, right, (((1,), (1,)), ((), ())), preferred_element_type=jnp.float32
            )
        acc = acc.astype(jnp.int32)
        code = acc[:64] | (acc[64:128] << 8) | (acc[128:] << BAG_SHIFT)
        out_ref[:, 4 * t : 4 * t + 4, :] = code.reshape(OWNERS, 4, 128)
    out_ref[:, 20:, :] = jnp.zeros((OWNERS, 4, 128), jnp.int32)


def pool_kernel(first, lists_ref, table_ref, out_ref, buf_ref, held_ref, rows_vmem, rows_ref, sem, row_sem):
    tables = held_ref.shape[0]
    turn, part = pl.program_id(0), pl.program_id(1)

    def load(t, k):
        piece = pl.ds(k * (ROWS_DEV // PIECES), ROWS_DEV // PIECES)
        return pltpu.make_async_copy(
            table_ref.at[first + t, piece], held_ref.at[t, piece], sem.at[t, k]
        )

    def load_rows():
        return pltpu.make_async_copy(rows_vmem, rows_ref, row_sem)

    @pl.when((turn == 0) & (part == 0))
    def _():
        for t in range(tables):
            for k in range(PIECES):
                load(t, k).start()
        codes = lists_ref[:, 4 * first : 4 * (first + tables), :]
        rows_vmem[:, : 4 * tables, :] = codes & (ROWS_DEV - 1)
        rows_vmem[:, 4 * tables : 5 * tables, :] = lists_ref[:, 16 + first : 16 + first + tables, :]
        load_rows().start()
        buf_ref[...] = jnp.zeros_like(buf_ref)
        load_rows().wait()

    for t in range(tables):

        @pl.when((turn == t) & (part == 0))
        def _(t=t):
            for k in range(PIECES):
                load(t, k).wait()

    def fetch(q, carry):
        source = part * STEP + q
        count = rows_ref[source, 4 * tables + turn, 0]
        for line in range(CAP // 128):
            for base in range(0, 128, BLOCK):

                @pl.when(count > line * 128 + base)
                def _(line=line, base=base):
                    for k in range(base, base + BLOCK):
                        row = rows_ref[source, 4 * turn + line, k]
                        buf_ref[q, pl.ds(line * 128 + k, 1), :] = held_ref[turn, pl.ds(row, 1), :]

        return carry

    lax.fori_loop(0, STEP, fetch, 0)
    bag = (iota((SAMPLES, 128), 0) + 1).astype(jnp.float32).astype(jnp.bfloat16)
    for q in range(STEP):
        source = part * STEP + q
        picks = []
        for line in range(CAP // 128):
            named = lists_ref[source, pl.ds(4 * first + 4 * turn + line, 1), :] >> BAG_SHIFT
            named = named.astype(jnp.float32).astype(jnp.bfloat16)
            picks.append(jnp.where(named == bag, jnp.bfloat16(1), jnp.bfloat16(0)))
        out_ref[q] = jnp.dot(
            jnp.concatenate(picks, axis=1),
            buf_ref[q].astype(jnp.bfloat16),
            preferred_element_type=jnp.float32,
        ).astype(out_ref.dtype)


def pool_tables(first, tables, lists, table):
    width = -(-5 * tables // 8) * 8
    return pl.pallas_call(
        functools.partial(pool_kernel, first),
        grid=(tables, OWNERS // STEP),
        in_specs=[
            pl.BlockSpec(lists.shape, lambda t, i: (0, 0, 0)),
            pl.BlockSpec(memory_space=pltpu.HBM),
        ],
        out_specs=pl.BlockSpec((STEP, SAMPLES, EMB), lambda t, i: (i, 0, t)),
        scratch_shapes=[
            pltpu.VMEM((STEP, CAP, EMB), jnp.float32),
            pltpu.VMEM((tables, ROWS_DEV, EMB), jnp.float32),
            pltpu.VMEM((OWNERS, width, 128), jnp.int32),
            pltpu.SMEM((OWNERS, width, 128), jnp.int32),
            pltpu.SemaphoreType.DMA((tables, PIECES)),
            pltpu.SemaphoreType.DMA(()),
        ],
        out_shape=jax.ShapeDtypeStruct((OWNERS, SAMPLES, tables * EMB), jnp.bfloat16),
        compiler_params=pltpu.CompilerParams(vmem_limit_bytes=49 << 20),
        cost_estimate=pl.CostEstimate(
            flops=10_000_000_000 * tables, transcendentals=0, bytes_accessed=6_000_000
        ),
    )(lists, table)


def score_kernel(pieces, chunks, *refs):
    features = refs[:chunks]
    biases = refs[chunks : chunks + pieces]
    w_in = refs[chunks + pieces : chunks + 2 * pieces]
    w_out = refs[chunks + 2 * pieces : chunks + 3 * pieces]
    out_ref, in_buf, out_buf, in_sem, out_sem = refs[chunks + 3 * pieces :]
    copies = []
    for p in range(pieces):
        first = pltpu.make_async_copy(w_in[p], in_buf.at[p], in_sem.at[p])
        second = pltpu.make_async_copy(w_out[p], out_buf.at[p], out_sem.at[p])
        first.start()
        second.start()
        copies.append((first, second))
    total = None
    for p in range(pieces):
        copies[p][0].wait()
        pre = biases[p][...]
        base = 0
        for feature in features:
            width = feature.shape[1]
            pre = pre + jnp.dot(
                feature[...],
                in_buf[p, base : base + width, :],
                preferred_element_type=jnp.float32,
            )
            base += width
        hidden = jnp.maximum(pre, 0.0).astype(jnp.bfloat16)
        copies[p][1].wait()
        part = jnp.dot(hidden, out_buf[p], preferred_element_type=jnp.float32)
        total = part if total is None else total + part
    out_ref[...] = total.astype(out_ref.dtype)


def score(features, biases, w_in, w_out, dtype):
    pieces, chunks = len(w_in), len(features)
    vmem = pl.BlockSpec(memory_space=pltpu.VMEM)
    hbm = pl.BlockSpec(memory_space=pltpu.HBM)
    return pl.pallas_call(
        functools.partial(score_kernel, pieces, chunks),
        in_specs=[vmem] * (chunks + pieces) + [hbm] * (2 * pieces),
        out_specs=vmem,
        scratch_shapes=[
            pltpu.VMEM((pieces, *w_in[0].shape), jnp.bfloat16),
            pltpu.VMEM((pieces, *w_out[0].shape), jnp.bfloat16),
            pltpu.SemaphoreType.DMA((pieces,)),
            pltpu.SemaphoreType.DMA((pieces,)),
        ],
        out_shape=jax.ShapeDtypeStruct((SAMPLES, w_out[0].shape[1]), dtype),
        compiler_params=pltpu.CompilerParams(vmem_limit_bytes=40 << 20),
        cost_estimate=pl.CostEstimate(
            flops=10_000_000_000, transcendentals=0, bytes_accessed=14_000_000
        ),
    )(*features, *biases, *w_in, *w_out)


def to_chip(array, targets):
    return lax.ppermute(
        array, "gy", [(x * 2 + c, targets[c](x) * 2 + c) for x in range(4) for c in range(2)]
    )


def flip(x):
    return x ^ 1


def mirror(x):
    return 3 - x


def to_core(array):
    return lax.ppermute(array, "gy", [(k, k ^ 1) for k in range(8)])


def local(table, lookup_owner, lookup_row, bag_length, top_in, top_bias, top_out):
    own = (top_bias.reshape(1, -1), top_in, top_out)
    near, far, far_near = [], [], []
    for k, array in enumerate(own):
        near.append(to_core(array))
        far.append(to_chip(array, (mirror, flip)))
        far_near.append(to_chip(near[k], (mirror, flip)))
    biases, w_in, w_out = zip(own, near, far, far_near)

    owner = jnp.transpose(lookup_owner[..., 0], (0, 2, 1))
    live = jnp.arange(BAG, dtype=jnp.int32)[None, :, None] < bag_length[:, None, :]
    owner = jnp.where(live, owner, OWNERS)
    row = jnp.transpose(lookup_row, (0, 2, 1))
    lists = pl.pallas_call(
        dispatch_kernel,
        out_shape=jax.ShapeDtypeStruct((OWNERS, 24, 128), jnp.int32),
        name="dispatch",
    )(owner, row)
    lists = lax.all_to_all(lists, "gx", 0, 0, tiled=True)

    mine, theirs = [], []
    first = 0
    for number in CHUNKS:
        share = pool_tables(first, number, lists, table)
        share = lax.all_to_all(share, "gx", 0, 0, tiled=True)
        chunk = jnp.sum(share.astype(jnp.float32), axis=0).astype(jnp.bfloat16)
        mine.append(chunk)
        theirs.append(to_chip(chunk, (flip, mirror)))
        first += number
    kept = score(mine, biases, w_in, w_out, jnp.float32)
    sent = score(theirs, biases, w_in, w_out, jnp.bfloat16)
    received = to_chip(sent, (flip, mirror))
    return (kept + received.astype(jnp.float32)).astype(jnp.bfloat16)


def solution(mesh):
    return jax.shard_map(
        local,
        mesh=mesh,
        in_specs=(
            P(None, "gx", None),
            P(None, ("gx", "gy"), None, None),
            P(None, ("gx", "gy"), None),
            P(None, ("gx", "gy")),
            P(None, "gy"),
            P("gy"),
            P("gy", None),
        ),
        out_specs=P(("gx", "gy"), None),
        check_vma=False,
    )
```

```python
import functools

import jax
import jax.numpy as jnp
from jax import lax
from jax.experimental import pallas as pl
from jax.experimental.pallas import tpu as pltpu
from jax.sharding import PartitionSpec as P


TABLES = 4
SAMPLES = 256
BAG = 16
OWNERS = 16
CAP = 512
ROWS_DEV = 8192
EMB = 128
BLOCK = 64
PIECES = 4
STEP = 8
BAG_SHIFT = 13
CHUNKS = (2, 2)


def iota(shape, dim):
    return lax.broadcasted_iota(jnp.int32, shape, dim)


def ones_where(mask):
    return jnp.where(mask, 1.0, 0.0).astype(jnp.bfloat16)


def dispatch_kernel(own_ref, row_ref, out_ref):
    before = ones_where(iota((256, 256), 0) < iota((256, 256), 1))
    r, c = iota((256, 256), 0), iota((256, 256), 1)
    earlier = ones_where(((r & 15) == (c & 15)) & ((c >> 4) < (r >> 4)))
    ones = jnp.ones((256, 256), jnp.bfloat16)
    same = ones_where(iota((16, 256), 0) == (iota((16, 256), 1) & 15))
    owner_iota = iota((16, 16, 256), 1)
    count64 = iota((64, 256), 0).astype(jnp.float32).astype(jnp.bfloat16)
    count128 = iota((128, 256), 0).astype(jnp.float32).astype(jnp.bfloat16)
    bag = (iota((1, 256), 1) + 1).astype(jnp.float32).astype(jnp.bfloat16)
    zero, one = jnp.bfloat16(0), jnp.bfloat16(1)
    own = own_ref[...]
    mark = (own[:, None, :] == owner_iota).reshape(256, 256)
    onehot = ones_where(mark)
    rank = jnp.dot(onehot, before, preferred_element_type=jnp.float32)
    lead = jnp.dot(earlier, onehot, preferred_element_type=jnp.float32)
    rank += jnp.dot(lead.astype(jnp.bfloat16), ones, preferred_element_type=jnp.float32)
    rank = jnp.sum(jnp.where(mark, rank, 0.0).reshape(16, 16, 256), axis=1).astype(jnp.int32)
    total = jnp.dot(same, onehot, preferred_element_type=jnp.float32)
    total = jnp.dot(total.astype(jnp.bfloat16), ones, preferred_element_type=jnp.float32)
    hi = (own * 4 + (rank >> 7)).astype(jnp.float32)
    lo = (rank & 127).astype(jnp.float32)
    row = row_ref[...]
    low = (row & 255).astype(jnp.float32)
    high = (row >> 8).astype(jnp.float32)
    acc = jnp.zeros((192, 128), jnp.float32)
    for s in range(BAG):
        line = slice(s, s + 1)
        left = hi[line].astype(jnp.bfloat16) == count64
        planes = jnp.concatenate(
            [
                jnp.where(left, low[line].astype(jnp.bfloat16), zero),
                jnp.where(left, high[line].astype(jnp.bfloat16), zero),
                jnp.where(left, bag, zero),
            ],
            axis=0,
        )
        right = jnp.where(lo[line].astype(jnp.bfloat16) == count128, one, zero)
        acc += lax.dot_general(
            planes, right, (((1,), (1,)), ((), ())), preferred_element_type=jnp.float32
        )
    acc = acc.astype(jnp.int32)
    code = acc[:64] | (acc[64:128] << 8) | (acc[128:] << BAG_SHIFT)
    out_ref[:, :4, :] = code.reshape(OWNERS, 4, 128)
    out_ref[:, 4, :] = total[:, :128].astype(jnp.int32)
    out_ref[:, 5:, :] = jnp.zeros((OWNERS, 3, 128), jnp.int32)


def pool_kernel(first, lists_ref, table_ref, out_ref, buf_ref, held_ref, rows_vmem, rows_ref, sem, row_sem):
    tables = held_ref.shape[0] // ROWS_DEV
    turn, part = pl.program_id(0), pl.program_id(1)

    def load(t, k):
        size = ROWS_DEV // PIECES
        return pltpu.make_async_copy(
            table_ref.at[first + t, pl.ds(k * size, size)],
            held_ref.at[pl.ds(t * ROWS_DEV + k * size, size)],
            sem.at[t, k],
        )

    def load_rows():
        return pltpu.make_async_copy(rows_vmem, rows_ref, row_sem)

    @pl.when((turn == 0) & (part == 0))
    def _():
        for t in range(tables):
            for k in range(PIECES):
                load(t, k).start()
        codes = lists_ref[:, 8 * first : 8 * (first + tables), :]
        line = iota(codes.shape, 1)
        rows = (codes & (ROWS_DEV - 1)) + (line >> 3) * ROWS_DEV
        rows_vmem[...] = jnp.where((line & 7) == 4, codes, rows)
        load_rows().start()
        buf_ref[...] = jnp.zeros_like(buf_ref)
        load_rows().wait()

    for t in range(tables):

        @pl.when((turn == t) & (part == 0))
        def _(t=t):
            for k in range(PIECES):
                load(t, k).wait()

    def fetch(q, carry):
        source = part * STEP + q
        count = rows_ref[source, 8 * turn + 4, 0]
        for line in range(CAP // 128):
            for base in range(0, 128, BLOCK):

                @pl.when(count > line * 128 + base)
                def _(line=line, base=base):
                    for k in range(base, base + BLOCK):
                        ids = rows_ref.at[source, 8 * turn + line, pl.ds(k // 8 * 8, 8)]
                        row = ids[k % 8]
                        buf_ref[q, pl.ds(line * 128 + k, 1), :] = held_ref[pl.ds(row, 1), :]

        return carry

    lax.fori_loop(0, STEP, fetch, 0)
    bag = (iota((SAMPLES, 128), 0) + 1).astype(jnp.float32).astype(jnp.bfloat16)
    for q in range(STEP):
        source = part * STEP + q
        picks = []
        for line in range(CAP // 128):
            named = lists_ref[source, pl.ds(8 * first + 8 * turn + line, 1), :] >> BAG_SHIFT
            named = named.astype(jnp.float32).astype(jnp.bfloat16)
            picks.append(jnp.where(named == bag, jnp.bfloat16(1), jnp.bfloat16(0)))
        out_ref[q] = jnp.dot(
            jnp.concatenate(picks, axis=1),
            buf_ref[q].astype(jnp.bfloat16),
            preferred_element_type=jnp.float32,
        ).astype(out_ref.dtype)


def pool_tables(first, tables, lists, table):
    return pl.pallas_call(
        functools.partial(pool_kernel, first),
        grid=(tables, OWNERS // STEP),
        in_specs=[
            pl.BlockSpec(lists.shape, lambda t, i: (0, 0, 0)),
            pl.BlockSpec(memory_space=pltpu.HBM),
        ],
        out_specs=pl.BlockSpec((STEP, SAMPLES, EMB), lambda t, i: (i, 0, t)),
        scratch_shapes=[
            pltpu.VMEM((STEP, CAP, EMB), jnp.float32),
            pltpu.VMEM((tables * ROWS_DEV, EMB), jnp.float32),
            pltpu.VMEM((OWNERS, 8 * tables, 128), jnp.int32),
            pltpu.SMEM((OWNERS, 8 * tables, 128), jnp.int32),
            pltpu.SemaphoreType.DMA((tables, PIECES)),
            pltpu.SemaphoreType.DMA(()),
        ],
        out_shape=jax.ShapeDtypeStruct((OWNERS, SAMPLES, tables * EMB), jnp.bfloat16),
        compiler_params=pltpu.CompilerParams(vmem_limit_bytes=104 << 19),
        cost_estimate=pl.CostEstimate(
            flops=10_000_000_000 * tables, transcendentals=0, bytes_accessed=6_000_000
        ),
    )(lists, table)


def add_kernel(shares_ref, out_ref):
    total = shares_ref[0].astype(jnp.float32)
    for k in range(1, OWNERS):
        total += shares_ref[k].astype(jnp.float32)
    out_ref[...] = total.astype(out_ref.dtype)


def add_shares(shares):
    width = shares.shape[2]
    return pl.pallas_call(
        add_kernel,
        grid=(4,),
        in_specs=[pl.BlockSpec((OWNERS, SAMPLES // 4, width), lambda i: (0, i, 0))],
        out_specs=pl.BlockSpec((SAMPLES // 4, width), lambda i: (i, 0)),
        out_shape=jax.ShapeDtypeStruct((SAMPLES, width), jnp.bfloat16),
        compiler_params=pltpu.CompilerParams(vmem_limit_bytes=12 << 20),
        name="add",
    )(shares)


def score_kernel(pieces, chunks, *refs):
    features = refs[:chunks]
    biases = refs[chunks : chunks + pieces]
    w_in = refs[chunks + pieces : chunks + 2 * pieces]
    w_out = refs[chunks + 2 * pieces : chunks + 3 * pieces]
    out_ref, in_buf, out_buf, in_sem, out_sem = refs[chunks + 3 * pieces :]
    copies = []
    for p in range(pieces):
        first = pltpu.make_async_copy(w_in[p], in_buf.at[p], in_sem.at[p])
        second = pltpu.make_async_copy(w_out[p], out_buf.at[p], out_sem.at[p])
        first.start()
        second.start()
        copies.append((first, second))
    total = None
    for p in range(pieces):
        copies[p][0].wait()
        pre = biases[p][...]
        base = 0
        for feature in features:
            width = feature.shape[1]
            pre = pre + jnp.dot(
                feature[...],
                in_buf[p, base : base + width, :],
                preferred_element_type=jnp.float32,
            )
            base += width
        hidden = jnp.maximum(pre, 0.0).astype(jnp.bfloat16)
        copies[p][1].wait()
        part = jnp.dot(hidden, out_buf[p], preferred_element_type=jnp.float32)
        total = part if total is None else total + part
    out_ref[...] = total.astype(out_ref.dtype)


def score(features, biases, w_in, w_out, dtype):
    pieces, chunks = len(w_in), len(features)
    vmem = pl.BlockSpec(memory_space=pltpu.VMEM)
    hbm = pl.BlockSpec(memory_space=pltpu.HBM)
    return pl.pallas_call(
        functools.partial(score_kernel, pieces, chunks),
        in_specs=[vmem] * (chunks + pieces) + [hbm] * (2 * pieces),
        out_specs=vmem,
        scratch_shapes=[
            pltpu.VMEM((pieces, *w_in[0].shape), jnp.bfloat16),
            pltpu.VMEM((pieces, *w_out[0].shape), jnp.bfloat16),
            pltpu.SemaphoreType.DMA((pieces,)),
            pltpu.SemaphoreType.DMA((pieces,)),
        ],
        out_shape=jax.ShapeDtypeStruct((SAMPLES, w_out[0].shape[1]), dtype),
        compiler_params=pltpu.CompilerParams(vmem_limit_bytes=40 << 20),
        cost_estimate=pl.CostEstimate(
            flops=10_000_000_000, transcendentals=0, bytes_accessed=14_000_000
        ),
    )(*features, *biases, *w_in, *w_out)


def to_chip(array, targets):
    return lax.ppermute(
        array, "gy", [(x * 2 + c, targets[c](x) * 2 + c) for x in range(4) for c in range(2)]
    )


def flip(x):
    return x ^ 1


def mirror(x):
    return 3 - x


def to_core(array):
    return lax.ppermute(array, "gy", [(k, k ^ 1) for k in range(8)])


def local(table, lookup_owner, lookup_row, bag_length, top_in, top_bias, top_out):
    own = (top_bias.reshape(1, -1), top_in, top_out)
    near, far, far_near = [], [], []
    for k, array in enumerate(own):
        near.append(to_core(array))
        far.append(to_chip(array, (mirror, flip)))
        far_near.append(to_chip(near[k], (mirror, flip)))
    biases, w_in, w_out = zip(own, near, far, far_near)

    owner = jnp.transpose(lookup_owner[..., 0], (0, 2, 1))
    live = jnp.arange(BAG, dtype=jnp.int32)[None, :, None] < bag_length[:, None, :]
    owner = jnp.where(live, owner, OWNERS)
    row = jnp.transpose(lookup_row, (0, 2, 1))
    lists = pl.pallas_call(
        dispatch_kernel,
        grid=(TABLES,),
        in_specs=[pl.BlockSpec((None, BAG, SAMPLES), lambda t: (t, 0, 0))] * 2,
        out_specs=pl.BlockSpec((OWNERS, 8, 128), lambda t: (0, t, 0)),
        out_shape=jax.ShapeDtypeStruct((OWNERS, 8 * TABLES, 128), jnp.int32),
        name="dispatch",
    )(owner, row)
    lists = lax.all_to_all(lists, "gx", 0, 0, tiled=True)

    mine, theirs = [], []
    first = 0
    for number in CHUNKS:
        share = pool_tables(first, number, lists, table)
        share = lax.all_to_all(share, "gx", 0, 0, tiled=True)
        chunk = add_shares(share)
        mine.append(chunk)
        theirs.append(to_chip(chunk, (flip, mirror)))
        first += number
    kept = score(mine, biases, w_in, w_out, jnp.float32)
    sent = score(theirs, biases, w_in, w_out, jnp.bfloat16)
    received = to_chip(sent, (flip, mirror))
    return (kept + received.astype(jnp.float32)).astype(jnp.bfloat16)


def solution(mesh):
    return jax.shard_map(
        local,
        mesh=mesh,
        in_specs=(
            P(None, "gx", None),
            P(None, ("gx", "gy"), None, None),
            P(None, ("gx", "gy"), None),
            P(None, ("gx", "gy")),
            P(None, "gy"),
            P("gy"),
            P("gy", None),
        ),
        out_specs=P(("gx", "gy"), None),
        check_vma=False,
    )
```

```python
import functools

import jax
import jax.numpy as jnp
from jax import lax
from jax.experimental import pallas as pl
from jax.experimental.pallas import tpu as pltpu
from jax.sharding import PartitionSpec as P


TABLES = 4
SAMPLES = 256
BAG = 16
OWNERS = 16
CAP = 512
ROWS_DEV = 8192
EMB = 128
BLOCK = 64
PIECES = 4
STEP = 8
BAG_SHIFT = 13
EACH = 1


def iota(shape, dim):
    return lax.broadcasted_iota(jnp.int32, shape, dim)


def ones_where(mask):
    return jnp.where(mask, 1.0, 0.0).astype(jnp.bfloat16)


def dispatch_kernel(own_ref, row_ref, length_ref, out_ref):
    before = ones_where(iota((256, 256), 0) < iota((256, 256), 1))
    r, c = iota((256, 256), 0), iota((256, 256), 1)
    earlier = ones_where(((r & 15) == (c & 15)) & ((c >> 4) < (r >> 4)))
    ones = jnp.ones((256, 256), jnp.bfloat16)
    same = ones_where(iota((16, 256), 0) == (iota((16, 256), 1) & 15))
    owner_iota = iota((16, 16, 256), 1)
    count64 = iota((64, 256), 0).astype(jnp.float32).astype(jnp.bfloat16)
    count128 = iota((128, 256), 0).astype(jnp.float32).astype(jnp.bfloat16)
    bag = (iota((1, 256), 1) + 1).astype(jnp.float32).astype(jnp.bfloat16)
    zero, one = jnp.bfloat16(0), jnp.bfloat16(1)
    for t in range(TABLES):
        live = iota((BAG, SAMPLES), 0) < length_ref[t : t + 1, :]
        own = jnp.where(live, own_ref[t], OWNERS)
        mark = (own[:, None, :] == owner_iota).reshape(256, 256)
        onehot = ones_where(mark)
        rank = jnp.dot(onehot, before, preferred_element_type=jnp.float32)
        lead = jnp.dot(earlier, onehot, preferred_element_type=jnp.float32)
        rank += jnp.dot(lead.astype(jnp.bfloat16), ones, preferred_element_type=jnp.float32)
        rank = jnp.sum(jnp.where(mark, rank, 0.0).reshape(16, 16, 256), axis=1).astype(jnp.int32)
        total = jnp.dot(same, onehot, preferred_element_type=jnp.float32)
        total = jnp.dot(total.astype(jnp.bfloat16), ones, preferred_element_type=jnp.float32)
        hi = (own * 4 + (rank >> 7)).astype(jnp.float32)
        lo = (rank & 127).astype(jnp.float32)
        row = row_ref[t]
        low = (row & 255).astype(jnp.float32)
        high = (row >> 8).astype(jnp.float32)
        acc = jnp.zeros((192, 128), jnp.float32)
        for s in range(BAG):
            line = slice(s, s + 1)
            left = hi[line].astype(jnp.bfloat16) == count64
            planes = jnp.concatenate(
                [
                    jnp.where(left, low[line].astype(jnp.bfloat16), zero),
                    jnp.where(left, high[line].astype(jnp.bfloat16), zero),
                    jnp.where(left, bag, zero),
                ],
                axis=0,
            )
            right = jnp.where(lo[line].astype(jnp.bfloat16) == count128, one, zero)
            acc += lax.dot_general(
                planes, right, (((1,), (1,)), ((), ())), preferred_element_type=jnp.float32
            )
        acc = acc.astype(jnp.int32)
        code = acc[:64] | (acc[64:128] << 8) | (acc[128:] << BAG_SHIFT)
        out_ref[:, 8 * t : 8 * t + 4, :] = code.reshape(OWNERS, 4, 128)
        out_ref[:, 8 * t + 4, :] = total[:, :128].astype(jnp.int32)
        out_ref[:, 8 * t + 5 : 8 * t + 8, :] = jnp.zeros((OWNERS, 3, 128), jnp.int32)


def pool_kernel(first, each, me_ref, lists_ref, table_ref, *refs):
    outs, (buf_ref, stage_ref, held_ref, rows_vmem, rows_ref, sem, row_sem, out_sem) = (
        refs[:8],
        refs[8:],
    )
    tables = 2 * each
    turn, part = pl.program_id(0), pl.program_id(1)
    my_y, my_z = me_ref[0] >> 2, me_ref[0] & 3

    def load(t, k):
        size = ROWS_DEV // PIECES
        return pltpu.make_async_copy(
            table_ref.at[first + t, pl.ds(k * size, size)],
            held_ref.at[pl.ds(t * ROWS_DEV + k * size, size)],
            sem.at[t, k],
        )

    def load_rows():
        return pltpu.make_async_copy(rows_vmem, rows_ref, row_sem)

    def unload(t, p, h):
        slot = (2 * t + p) % 2
        columns = pl.ds(t % each * EMB, EMB)
        return pltpu.make_async_copy(
            stage_ref.at[slot, pl.ds(4 * h, 4)],
            outs[4 * (t // each) + 2 * p + h].at[:, :, columns],
            out_sem.at[slot, h],
        )

    def source_of(place):
        outer, inner = place >> 2, place & 3
        step_y = jnp.where(turn < each, outer, inner)
        step_z = jnp.where(turn < each, inner, outer)
        return (((my_y + step_y) & 3) << 2) + ((my_z + step_z) & 3)

    @pl.when((turn == 0) & (part == 0))
    def _():
        for t in range(tables):
            for k in range(PIECES):
                load(t, k).start()
        codes = lists_ref[:, 8 * first : 8 * (first + tables), :]
        line = iota(codes.shape, 1)
        rows = (codes & (ROWS_DEV - 1)) + (line >> 3) * ROWS_DEV
        rows_vmem[...] = jnp.where((line & 7) == 4, codes, rows)
        load_rows().start()
        buf_ref[...] = jnp.zeros_like(buf_ref)
        load_rows().wait()

    for t in range(tables):

        @pl.when((turn == t) & (part == 0))
        def _(t=t):
            for k in range(PIECES):
                load(t, k).wait()

    def fetch(q, carry):
        source = source_of(part * STEP + q)
        count = rows_ref[source, 8 * turn + 4, 0]
        for line in range(CAP // 128):
            for base in range(0, 128, BLOCK):

                @pl.when(count > line * 128 + base)
                def _(line=line, base=base):
                    for k in range(base, base + BLOCK):
                        ids = rows_ref.at[source, 8 * turn + line, pl.ds(k // 8 * 8, 8)]
                        row = ids[k % 8]
                        buf_ref[q, pl.ds(line * 128 + k, 1), :] = held_ref[pl.ds(row, 1), :]

        return carry

    lax.fori_loop(0, STEP, fetch, 0)
    for t in range(1, tables):
        for p in range(2):

            @pl.when((turn == t) & (part == p))
            def _(t=t, p=p):
                for h in range(2):
                    unload(t - 1, p, h).wait()

    bag = (iota((SAMPLES, 128), 0) + 1).astype(jnp.float32).astype(jnp.bfloat16)
    for q in range(STEP):
        source = source_of(part * STEP + q)
        picks = []
        for line in range(CAP // 128):
            named = lists_ref[source, pl.ds(8 * first + 8 * turn + line, 1), :] >> BAG_SHIFT
            named = named.astype(jnp.float32).astype(jnp.bfloat16)
            picks.append(jnp.where(named == bag, jnp.bfloat16(1), jnp.bfloat16(0)))
        stage_ref[part, q] = jnp.dot(
            jnp.concatenate(picks, axis=1),
            buf_ref[q].astype(jnp.bfloat16),
            preferred_element_type=jnp.float32,
        ).astype(stage_ref.dtype)
    for t in range(tables):
        for p in range(2):

            @pl.when((turn == t) & (part == p))
            def _(t=t, p=p):
                for h in range(2):
                    unload(t, p, h).start()
                if t == tables - 1 and p == 1:
                    for h in range(2):
                        unload(t, 0, h).wait()
                    for h in range(2):
                        unload(t, 1, h).wait()


def pool_tables(first, each, me, lists, table):
    tables = 2 * each
    vmem = pl.BlockSpec(memory_space=pltpu.VMEM)
    hbm = pl.BlockSpec(memory_space=pltpu.HBM)
    return pl.pallas_call(
        functools.partial(pool_kernel, first, each),
        grid=(tables, OWNERS // STEP),
        in_specs=[pl.BlockSpec(memory_space=pltpu.SMEM), vmem, hbm],
        out_specs=[hbm] * 8,
        scratch_shapes=[
            pltpu.VMEM((STEP, CAP, EMB), jnp.float32),
            pltpu.VMEM((2, STEP, SAMPLES, EMB), jnp.bfloat16),
            pltpu.VMEM((tables * ROWS_DEV, EMB), jnp.float32),
            pltpu.VMEM((OWNERS, 8 * tables, 128), jnp.int32),
            pltpu.SMEM((OWNERS, 8 * tables, 128), jnp.int32),
            pltpu.SemaphoreType.DMA((tables, PIECES)),
            pltpu.SemaphoreType.DMA(()),
            pltpu.SemaphoreType.DMA((2, 2)),
        ],
        out_shape=[jax.ShapeDtypeStruct((4, SAMPLES, each * EMB), jnp.bfloat16)] * 8,
        compiler_params=pltpu.CompilerParams(vmem_limit_bytes=48 << 20),
        cost_estimate=pl.CostEstimate(
            flops=10_000_000_000 * tables, transcendentals=0, bytes_accessed=6_000_000
        ),
    )(me, lists, table)


def add_first_kernel(*refs):
    ins, outs = refs[:8], refs[8:]
    for half in range(2):
        for k in range(4):
            total = ins[4 * half][k].astype(jnp.float32)
            for d in range(1, 4):
                total += ins[4 * half + d][k].astype(jnp.float32)
            outs[4 * half + k][...] = total.astype(jnp.bfloat16)


def add_first(parts):
    vmem = pl.BlockSpec(memory_space=pltpu.VMEM)
    return pl.pallas_call(
        add_first_kernel,
        in_specs=[vmem] * 8,
        out_specs=[vmem] * 8,
        out_shape=[jax.ShapeDtypeStruct(parts[0].shape[1:], jnp.bfloat16)] * 8,
        compiler_params=pltpu.CompilerParams(vmem_limit_bytes=16 << 20),
        name="add_first",
    )(*parts)


def add_second_kernel(*refs):
    ins, out_ref = refs[:8], refs[8]
    width = ins[0].shape[1]
    for half in range(2):
        total = ins[4 * half][...].astype(jnp.float32)
        for d in range(1, 4):
            total += ins[4 * half + d][...].astype(jnp.float32)
        out_ref[:, half * width : (half + 1) * width] = total.astype(jnp.bfloat16)


def add_second(parts):
    vmem = pl.BlockSpec(memory_space=pltpu.VMEM)
    rows, width = parts[0].shape
    return pl.pallas_call(
        add_second_kernel,
        in_specs=[vmem] * 8,
        out_specs=vmem,
        out_shape=jax.ShapeDtypeStruct((rows, 2 * width), jnp.bfloat16),
        compiler_params=pltpu.CompilerParams(vmem_limit_bytes=16 << 20),
        name="add_second",
    )(*parts)


def score_kernel(pieces, chunks, *refs):
    features = refs[:chunks]
    biases = refs[chunks : chunks + pieces]
    w_in = refs[chunks + pieces : chunks + 2 * pieces]
    w_out = refs[chunks + 2 * pieces : chunks + 3 * pieces]
    out_ref, in_buf, out_buf, in_sem, out_sem = refs[chunks + 3 * pieces :]
    copies = []
    for p in range(pieces):
        first = pltpu.make_async_copy(w_in[p], in_buf.at[p], in_sem.at[p])
        second = pltpu.make_async_copy(w_out[p], out_buf.at[p], out_sem.at[p])
        first.start()
        second.start()
        copies.append((first, second))
    total = None
    for p in range(pieces):
        copies[p][0].wait()
        pre = biases[p][...]
        base = 0
        for feature in features:
            width = feature.shape[1]
            pre = pre + jnp.dot(
                feature[...],
                in_buf[p, base : base + width, :],
                preferred_element_type=jnp.float32,
            )
            base += width
        hidden = jnp.maximum(pre, 0.0).astype(jnp.bfloat16)
        copies[p][1].wait()
        part = jnp.dot(hidden, out_buf[p], preferred_element_type=jnp.float32)
        total = part if total is None else total + part
    out_ref[...] = total.astype(out_ref.dtype)


def score(features, biases, w_in, w_out, dtype):
    pieces, chunks = len(w_in), len(features)
    vmem = pl.BlockSpec(memory_space=pltpu.VMEM)
    hbm = pl.BlockSpec(memory_space=pltpu.HBM)
    return pl.pallas_call(
        functools.partial(score_kernel, pieces, chunks),
        in_specs=[vmem] * (chunks + pieces) + [hbm] * (2 * pieces),
        out_specs=vmem,
        scratch_shapes=[
            pltpu.VMEM((pieces, *w_in[0].shape), jnp.bfloat16),
            pltpu.VMEM((pieces, *w_out[0].shape), jnp.bfloat16),
            pltpu.SemaphoreType.DMA((pieces,)),
            pltpu.SemaphoreType.DMA((pieces,)),
        ],
        out_shape=jax.ShapeDtypeStruct((SAMPLES, w_out[0].shape[1]), dtype),
        compiler_params=pltpu.CompilerParams(vmem_limit_bytes=40 << 20),
        cost_estimate=pl.CostEstimate(
            flops=10_000_000_000, transcendentals=0, bytes_accessed=14_000_000
        ),
    )(*features, *biases, *w_in, *w_out)


def to_chip(array, targets):
    return lax.ppermute(
        array, "gy", [(x * 2 + c, targets[c](x) * 2 + c) for x in range(4) for c in range(2)]
    )


def flip(x):
    return x ^ 1


def mirror(x):
    return 3 - x


def along(array, axis, shift):
    if axis == "y":
        pairs = [(y * 4 + z, (y + shift) % 4 * 4 + z) for y in range(4) for z in range(4)]
    else:
        pairs = [(y * 4 + z, y * 4 + (z + shift) % 4) for y in range(4) for z in range(4)]
    return lax.ppermute(array, "gx", pairs)


def moved(parts, axes):
    out = list(parts)
    for shift in (2, 1, 3):
        for half in range(2):
            out[4 * half + shift] = along(parts[4 * half + shift], axes[half], shift)
    return out


def to_core(array):
    return lax.ppermute(array, "gy", [(k, k ^ 1) for k in range(8)])


def local(table, lookup_owner, lookup_row, bag_length, top_in, top_bias, top_out):
    own = (top_bias.reshape(1, -1), top_in, top_out)
    near, far, far_near = [], [], []
    for k, array in enumerate(own):
        near.append(to_core(array))
        far.append(to_chip(array, (mirror, flip)))
        far_near.append(to_chip(near[k], (mirror, flip)))
    biases, w_in, w_out = zip(own, near, far, far_near)

    owner = jnp.transpose(lookup_owner[..., 0], (0, 2, 1))
    row = jnp.transpose(lookup_row, (0, 2, 1))
    lists = pl.pallas_call(
        dispatch_kernel,
        out_shape=jax.ShapeDtypeStruct((OWNERS, 8 * TABLES, 128), jnp.int32),
        name="dispatch",
    )(owner, row, bag_length)
    lists = lax.all_to_all(lists, "gx", 0, 0, tiled=True)

    me = lax.axis_index("gx").astype(jnp.int32).reshape(1)
    mine, theirs = [], []
    for first in range(0, TABLES, 2 * EACH):
        parts = pool_tables(first, EACH, me, lists, table)
        parts = moved(parts, "yz")
        parts = add_first(parts)
        parts = moved(parts, "zy")
        chunk = add_second(parts)
        mine.append(chunk)
        theirs.append(to_chip(chunk, (flip, mirror)))
    kept = score(mine, biases, w_in, w_out, jnp.float32)
    sent = score(theirs, biases, w_in, w_out, jnp.bfloat16)
    received = to_chip(sent, (flip, mirror))
    return (kept + received.astype(jnp.float32)).astype(jnp.bfloat16)


def solution(mesh):
    return jax.shard_map(
        local,
        mesh=mesh,
        in_specs=(
            P(None, "gx", None),
            P(None, ("gx", "gy"), None, None),
            P(None, ("gx", "gy"), None),
            P(None, ("gx", "gy")),
            P(None, "gy"),
            P("gy"),
            P("gy", None),
        ),
        out_specs=P(("gx", "gy"), None),
        check_vma=False,
    )
```

```python
import functools

import jax
import jax.numpy as jnp
from jax import lax
from jax.experimental import pallas as pl
from jax.experimental.pallas import tpu as pltpu
from jax.sharding import PartitionSpec as P


TABLES = 4
SAMPLES = 256
BAG = 16
OWNERS = 16
CAP = 512
ROWS_DEV = 8192
EMB = 128
BLOCK = 64
PIECES = 4
STEP = 8
BAG_SHIFT = 13
EACH = 1


def iota(shape, dim):
    return lax.broadcasted_iota(jnp.int32, shape, dim)


def ones_where(mask):
    return jnp.where(mask, 1.0, 0.0).astype(jnp.bfloat16)


def dispatch_kernel(own_ref, row_ref, length_ref, out_ref):
    before = ones_where(iota((256, 256), 0) < iota((256, 256), 1))
    r, c = iota((256, 256), 0), iota((256, 256), 1)
    earlier = ones_where(((r & 15) == (c & 15)) & ((c >> 4) < (r >> 4)))
    ones = jnp.ones((256, 256), jnp.bfloat16)
    same = ones_where(iota((16, 256), 0) == (iota((16, 256), 1) & 15))
    owner_iota = iota((16, 16, 256), 1)
    count64 = iota((64, 256), 0).astype(jnp.float32).astype(jnp.bfloat16)
    count128 = iota((128, 256), 0).astype(jnp.float32).astype(jnp.bfloat16)
    bag = (iota((1, 256), 1) + 1).astype(jnp.float32).astype(jnp.bfloat16)
    zero, one = jnp.bfloat16(0), jnp.bfloat16(1)
    for t in range(TABLES):
        live = iota((BAG, SAMPLES), 0) < length_ref[t : t + 1, :]
        own = jnp.where(live, own_ref[t], OWNERS)
        mark = (own[:, None, :] == owner_iota).reshape(256, 256)
        onehot = ones_where(mark)
        rank = jnp.dot(onehot, before, preferred_element_type=jnp.float32)
        lead = jnp.dot(earlier, onehot, preferred_element_type=jnp.float32)
        rank += jnp.dot(lead.astype(jnp.bfloat16), ones, preferred_element_type=jnp.float32)
        rank = jnp.sum(jnp.where(mark, rank, 0.0).reshape(16, 16, 256), axis=1).astype(jnp.int32)
        total = jnp.dot(same, onehot, preferred_element_type=jnp.float32)
        total = jnp.dot(total.astype(jnp.bfloat16), ones, preferred_element_type=jnp.float32)
        hi = (own * 4 + (rank >> 7)).astype(jnp.float32)
        lo = (rank & 127).astype(jnp.float32)
        row = row_ref[t]
        low = (row & 255).astype(jnp.float32)
        high = (row >> 8).astype(jnp.float32)
        acc = jnp.zeros((192, 128), jnp.float32)
        for s in range(BAG):
            line = slice(s, s + 1)
            left = hi[line].astype(jnp.bfloat16) == count64
            planes = jnp.concatenate(
                [
                    jnp.where(left, low[line].astype(jnp.bfloat16), zero),
                    jnp.where(left, high[line].astype(jnp.bfloat16), zero),
                    jnp.where(left, bag, zero),
                ],
                axis=0,
            )
            right = jnp.where(lo[line].astype(jnp.bfloat16) == count128, one, zero)
            acc += lax.dot_general(
                planes, right, (((1,), (1,)), ((), ())), preferred_element_type=jnp.float32
            )
        acc = acc.astype(jnp.int32)
        code = acc[:64] | (acc[64:128] << 8) | (acc[128:] << BAG_SHIFT)
        out_ref[:, 8 * t : 8 * t + 4, :] = code.reshape(OWNERS, 4, 128)
        out_ref[:, 8 * t + 4, :] = total[:, :128].astype(jnp.int32)
        out_ref[:, 8 * t + 5 : 8 * t + 8, :] = jnp.zeros((OWNERS, 3, 128), jnp.int32)


def pool_kernel(first, each, me_ref, lists_ref, table_ref, *refs):
    outs, (buf_ref, stage_ref, held_ref, rows_vmem, rows_ref, sem, row_sem, out_sem) = (
        refs[:8],
        refs[8:],
    )
    tables = 2 * each
    turn, part = pl.program_id(0), pl.program_id(1)
    my_y, my_z = me_ref[0] >> 2, me_ref[0] & 3

    def load(t, k):
        size = ROWS_DEV // PIECES
        return pltpu.make_async_copy(
            table_ref.at[first + t, pl.ds(k * size, size)],
            held_ref.at[pl.ds(t * ROWS_DEV + k * size, size)],
            sem.at[t, k],
        )

    def load_rows():
        return pltpu.make_async_copy(rows_vmem, rows_ref, row_sem)

    def unload(t, p, h):
        slot = (2 * t + p) % 2
        columns = pl.ds(t % each * EMB, EMB)
        return pltpu.make_async_copy(
            stage_ref.at[slot, pl.ds(4 * h, 4)],
            outs[4 * (t // each) + 2 * p + h].at[:, :, columns],
            out_sem.at[slot, h],
        )

    def source_of(place):
        outer, inner = place >> 2, place & 3
        step_y = jnp.where(turn < each, outer, inner)
        step_z = jnp.where(turn < each, inner, outer)
        return (((my_y + step_y) & 3) << 2) + ((my_z + step_z) & 3)

    @pl.when((turn == 0) & (part == 0))
    def _():
        for k in range(PIECES):
            load(0, k).start()
        codes = lists_ref[:, 8 * first : 8 * (first + tables), :]
        line = iota(codes.shape, 1)
        rows = (codes & (ROWS_DEV - 1)) + (line >> 3) * ROWS_DEV
        rows_vmem[...] = jnp.where((line & 7) == 4, codes, rows)
        load_rows().start()
        buf_ref[...] = jnp.zeros_like(buf_ref)
        load_rows().wait()

    for t in range(tables):

        @pl.when((turn == t) & (part == 0))
        def _(t=t):
            for k in range(PIECES):
                load(t, k).wait()
            if t + 1 < tables:
                for k in range(PIECES):
                    load(t + 1, k).start()

    def fetch(q, carry):
        source = source_of(part * STEP + q)
        count = rows_ref[source, 8 * turn + 4, 0]
        for line in range(CAP // 128):
            for base in range(0, 128, BLOCK):

                @pl.when(count > line * 128 + base)
                def _(line=line, base=base):
                    for k in range(base, base + BLOCK):
                        ids = rows_ref.at[source, 8 * turn + line, pl.ds(k // 8 * 8, 8)]
                        row = ids[k % 8]
                        buf_ref[q, pl.ds(line * 128 + k, 1), :] = held_ref[pl.ds(row, 1), :]

        return carry

    lax.fori_loop(0, STEP, fetch, 0)
    for t in range(1, tables):
        for p in range(2):

            @pl.when((turn == t) & (part == p))
            def _(t=t, p=p):
                for h in range(2):
                    unload(t - 1, p, h).wait()

    bag = (iota((SAMPLES, 128), 0) + 1).astype(jnp.float32).astype(jnp.bfloat16)
    for q in range(STEP):
        source = source_of(part * STEP + q)
        picks = []
        for line in range(CAP // 128):
            named = lists_ref[source, pl.ds(8 * first + 8 * turn + line, 1), :] >> BAG_SHIFT
            named = named.astype(jnp.float32).astype(jnp.bfloat16)
            picks.append(jnp.where(named == bag, jnp.bfloat16(1), jnp.bfloat16(0)))
        stage_ref[part, q] = jnp.dot(
            jnp.concatenate(picks, axis=1),
            buf_ref[q].astype(jnp.bfloat16),
            preferred_element_type=jnp.float32,
        ).astype(stage_ref.dtype)
    for t in range(tables):
        for p in range(2):

            @pl.when((turn == t) & (part == p))
            def _(t=t, p=p):
                for h in range(2):
                    unload(t, p, h).start()
                if t == tables - 1 and p == 1:
                    for h in range(2):
                        unload(t, 0, h).wait()
                    for h in range(2):
                        unload(t, 1, h).wait()


def pool_tables(first, each, me, lists, table):
    tables = 2 * each
    vmem = pl.BlockSpec(memory_space=pltpu.VMEM)
    hbm = pl.BlockSpec(memory_space=pltpu.HBM)
    return pl.pallas_call(
        functools.partial(pool_kernel, first, each),
        grid=(tables, OWNERS // STEP),
        in_specs=[pl.BlockSpec(memory_space=pltpu.SMEM), vmem, hbm],
        out_specs=[hbm] * 8,
        scratch_shapes=[
            pltpu.VMEM((STEP, CAP, EMB), jnp.float32),
            pltpu.VMEM((2, STEP, SAMPLES, EMB), jnp.bfloat16),
            pltpu.VMEM((tables * ROWS_DEV, EMB), jnp.float32),
            pltpu.VMEM((OWNERS, 8 * tables, 128), jnp.int32),
            pltpu.SMEM((OWNERS, 8 * tables, 128), jnp.int32),
            pltpu.SemaphoreType.DMA((tables, PIECES)),
            pltpu.SemaphoreType.DMA(()),
            pltpu.SemaphoreType.DMA((2, 2)),
        ],
        out_shape=[jax.ShapeDtypeStruct((4, SAMPLES, each * EMB), jnp.bfloat16)] * 8,
        compiler_params=pltpu.CompilerParams(vmem_limit_bytes=48 << 20),
        cost_estimate=pl.CostEstimate(
            flops=10_000_000_000 * tables, transcendentals=0, bytes_accessed=6_000_000
        ),
    )(me, lists, table)


def add_first_kernel(*refs):
    ins, outs = refs[:8], refs[8:]
    for half in range(2):
        for k in range(4):
            total = ins[4 * half][k].astype(jnp.float32)
            for d in range(1, 4):
                total += ins[4 * half + d][k].astype(jnp.float32)
            outs[4 * half + k][...] = total.astype(jnp.bfloat16)


def add_first(parts):
    vmem = pl.BlockSpec(memory_space=pltpu.VMEM)
    return pl.pallas_call(
        add_first_kernel,
        in_specs=[vmem] * 8,
        out_specs=[vmem] * 8,
        out_shape=[jax.ShapeDtypeStruct(parts[0].shape[1:], jnp.bfloat16)] * 8,
        compiler_params=pltpu.CompilerParams(vmem_limit_bytes=16 << 20),
        name="add_first",
    )(*parts)


def add_second_kernel(*refs):
    ins, out_ref = refs[:8], refs[8]
    width = ins[0].shape[1]
    for half in range(2):
        total = ins[4 * half][...].astype(jnp.float32)
        for d in range(1, 4):
            total += ins[4 * half + d][...].astype(jnp.float32)
        out_ref[:, half * width : (half + 1) * width] = total.astype(jnp.bfloat16)


def add_second(parts):
    vmem = pl.BlockSpec(memory_space=pltpu.VMEM)
    rows, width = parts[0].shape
    return pl.pallas_call(
        add_second_kernel,
        in_specs=[vmem] * 8,
        out_specs=vmem,
        out_shape=jax.ShapeDtypeStruct((rows, 2 * width), jnp.bfloat16),
        compiler_params=pltpu.CompilerParams(vmem_limit_bytes=16 << 20),
        name="add_second",
    )(*parts)


def score_kernel(pieces, chunks, *refs):
    features = refs[:chunks]
    biases = refs[chunks : chunks + pieces]
    w_in = refs[chunks + pieces : chunks + 2 * pieces]
    w_out = refs[chunks + 2 * pieces : chunks + 3 * pieces]
    out_ref, in_buf, out_buf, in_sem, out_sem = refs[chunks + 3 * pieces :]
    copies = []
    for p in range(pieces):
        first = pltpu.make_async_copy(w_in[p], in_buf.at[p], in_sem.at[p])
        second = pltpu.make_async_copy(w_out[p], out_buf.at[p], out_sem.at[p])
        first.start()
        second.start()
        copies.append((first, second))
    total = None
    for p in range(pieces):
        copies[p][0].wait()
        pre = biases[p][...]
        base = 0
        for feature in features:
            width = feature.shape[1]
            pre = pre + jnp.dot(
                feature[...],
                in_buf[p, base : base + width, :],
                preferred_element_type=jnp.float32,
            )
            base += width
        hidden = jnp.maximum(pre, 0.0).astype(jnp.bfloat16)
        copies[p][1].wait()
        part = jnp.dot(hidden, out_buf[p], preferred_element_type=jnp.float32)
        total = part if total is None else total + part
    out_ref[...] = total.astype(out_ref.dtype)


def score(features, biases, w_in, w_out, dtype):
    pieces, chunks = len(w_in), len(features)
    vmem = pl.BlockSpec(memory_space=pltpu.VMEM)
    hbm = pl.BlockSpec(memory_space=pltpu.HBM)
    return pl.pallas_call(
        functools.partial(score_kernel, pieces, chunks),
        in_specs=[vmem] * (chunks + pieces) + [hbm] * (2 * pieces),
        out_specs=vmem,
        scratch_shapes=[
            pltpu.VMEM((pieces, *w_in[0].shape), jnp.bfloat16),
            pltpu.VMEM((pieces, *w_out[0].shape), jnp.bfloat16),
            pltpu.SemaphoreType.DMA((pieces,)),
            pltpu.SemaphoreType.DMA((pieces,)),
        ],
        out_shape=jax.ShapeDtypeStruct((SAMPLES, w_out[0].shape[1]), dtype),
        compiler_params=pltpu.CompilerParams(vmem_limit_bytes=40 << 20),
        cost_estimate=pl.CostEstimate(
            flops=10_000_000_000, transcendentals=0, bytes_accessed=14_000_000
        ),
    )(*features, *biases, *w_in, *w_out)


def to_chip(array, targets):
    return lax.ppermute(
        array, "gy", [(x * 2 + c, targets[c](x) * 2 + c) for x in range(4) for c in range(2)]
    )


def flip(x):
    return x ^ 1


def mirror(x):
    return 3 - x


def along(array, axis, shift):
    if axis == "y":
        pairs = [(y * 4 + z, (y + shift) % 4 * 4 + z) for y in range(4) for z in range(4)]
    else:
        pairs = [(y * 4 + z, y * 4 + (z + shift) % 4) for y in range(4) for z in range(4)]
    return lax.ppermute(array, "gx", pairs)


def moved(parts, axes):
    out = list(parts)
    for shift in (2, 1, 3):
        for half in range(2):
            out[4 * half + shift] = along(parts[4 * half + shift], axes[half], shift)
    return out


def to_core(array):
    return lax.ppermute(array, "gy", [(k, k ^ 1) for k in range(8)])


def local(table, lookup_owner, lookup_row, bag_length, top_in, top_bias, top_out):
    own = (top_bias.reshape(1, -1), top_in, top_out)
    near, far, far_near = [], [], []
    for k, array in enumerate(own):
        near.append(to_core(array))
        far.append(to_chip(array, (mirror, flip)))
        far_near.append(to_chip(near[k], (mirror, flip)))
    biases, w_in, w_out = zip(own, near, far, far_near)

    owner = jnp.transpose(lookup_owner[..., 0], (0, 2, 1))
    row = jnp.transpose(lookup_row, (0, 2, 1))
    lists = pl.pallas_call(
        dispatch_kernel,
        out_shape=jax.ShapeDtypeStruct((OWNERS, 8 * TABLES, 128), jnp.int32),
        name="dispatch",
    )(owner, row, bag_length)
    lists = lax.all_to_all(lists, "gx", 0, 0, tiled=True)

    me = lax.axis_index("gx").astype(jnp.int32).reshape(1)
    mine, theirs = [], []
    for first in range(0, TABLES, 2 * EACH):
        parts = pool_tables(first, EACH, me, lists, table)
        parts = moved(parts, "yz")
        parts = add_first(parts)
        parts = moved(parts, "zy")
        chunk = add_second(parts)
        mine.append(chunk)
        theirs.append(to_chip(chunk, (flip, mirror)))
    kept = score(mine, biases, w_in, w_out, jnp.float32)
    sent = score(theirs, biases, w_in, w_out, jnp.bfloat16)
    received = to_chip(sent, (flip, mirror))
    return (kept + received.astype(jnp.float32)).astype(jnp.bfloat16)


def solution(mesh):
    return jax.shard_map(
        local,
        mesh=mesh,
        in_specs=(
            P(None, "gx", None),
            P(None, ("gx", "gy"), None, None),
            P(None, ("gx", "gy"), None),
            P(None, ("gx", "gy")),
            P(None, "gy"),
            P("gy"),
            P("gy", None),
        ),
        out_specs=P(("gx", "gy"), None),
        check_vma=False,
    )
```

```python
import functools

import jax
import jax.numpy as jnp
from jax import lax
from jax.experimental import pallas as pl
from jax.experimental.pallas import tpu as pltpu
from jax.sharding import PartitionSpec as P


TABLES = 4
SAMPLES = 256
BAG = 16
OWNERS = 16
CAP = 512
ROWS_DEV = 8192
EMB = 128
BLOCK = 64
PIECES = 4
STEP = 8
BAG_SHIFT = 13


def iota(shape, dim):
    return lax.broadcasted_iota(jnp.int32, shape, dim)


def ones_where(mask):
    return jnp.where(mask, 1.0, 0.0).astype(jnp.bfloat16)


def dispatch_kernel(own_ref, row_ref, length_ref, out_ref):
    before = ones_where(iota((256, 256), 0) < iota((256, 256), 1))
    r, c = iota((256, 256), 0), iota((256, 256), 1)
    earlier = ones_where(((r & 15) == (c & 15)) & ((c >> 4) < (r >> 4)))
    ones = jnp.ones((256, 256), jnp.bfloat16)
    same = ones_where(iota((16, 256), 0) == (iota((16, 256), 1) & 15))
    owner_iota = iota((16, 16, 256), 1)
    count64 = iota((64, 256), 0).astype(jnp.float32).astype(jnp.bfloat16)
    count128 = iota((128, 256), 0).astype(jnp.float32).astype(jnp.bfloat16)
    bag = (iota((1, 256), 1) + 1).astype(jnp.float32).astype(jnp.bfloat16)
    zero, one = jnp.bfloat16(0), jnp.bfloat16(1)
    for t in range(TABLES):
        live = iota((BAG, SAMPLES), 0) < length_ref[t : t + 1, :]
        own = jnp.where(live, own_ref[t, :, 0, :], OWNERS)
        mark = (own[:, None, :] == owner_iota).reshape(256, 256)
        onehot = ones_where(mark)
        rank = jnp.dot(onehot, before, preferred_element_type=jnp.float32)
        lead = jnp.dot(earlier, onehot, preferred_element_type=jnp.float32)
        rank += jnp.dot(lead.astype(jnp.bfloat16), ones, preferred_element_type=jnp.float32)
        rank = jnp.sum(jnp.where(mark, rank, 0.0).reshape(16, 16, 256), axis=1).astype(jnp.int32)
        total = jnp.dot(same, onehot, preferred_element_type=jnp.float32)
        total = jnp.dot(total.astype(jnp.bfloat16), ones, preferred_element_type=jnp.float32)
        hi = (own * 4 + (rank >> 7)).astype(jnp.float32)
        lo = (rank & 127).astype(jnp.float32)
        row = row_ref[t]
        low = (row & 255).astype(jnp.float32)
        high = (row >> 8).astype(jnp.float32)
        acc = jnp.zeros((192, 128), jnp.float32)
        for s in range(BAG):
            line = slice(s, s + 1)
            left = hi[line].astype(jnp.bfloat16) == count64
            planes = jnp.concatenate(
                [
                    jnp.where(left, low[line].astype(jnp.bfloat16), zero),
                    jnp.where(left, high[line].astype(jnp.bfloat16), zero),
                    jnp.where(left, bag, zero),
                ],
                axis=0,
            )
            right = jnp.where(lo[line].astype(jnp.bfloat16) == count128, one, zero)
            acc += lax.dot_general(
                planes, right, (((1,), (1,)), ((), ())), preferred_element_type=jnp.float32
            )
        acc = acc.astype(jnp.int32)
        code = acc[:64] | (acc[64:128] << 8) | (acc[128:] << BAG_SHIFT)
        out_ref[:, 8 * t : 8 * t + 4, :] = code.reshape(OWNERS, 4, 128)
        out_ref[:, 8 * t + 4, :] = total[:, :128].astype(jnp.int32)
        out_ref[:, 8 * t + 5 : 8 * t + 8, :] = jnp.zeros((OWNERS, 3, 128), jnp.int32)


def pool_kernel(first, each, me_ref, lists_ref, table_ref, *refs):
    outs, (buf_ref, stage_ref, held_ref, rows_vmem, rows_ref, sem, row_sem, out_sem) = (
        refs[:8],
        refs[8:],
    )
    tables = 2 * each
    turn, part = pl.program_id(0), pl.program_id(1)
    my_y, my_z = me_ref[0] >> 2, me_ref[0] & 3

    def load(t, k):
        size = ROWS_DEV // PIECES
        return pltpu.make_async_copy(
            table_ref.at[first + t, pl.ds(k * size, size)],
            held_ref.at[pl.ds(t * ROWS_DEV + k * size, size)],
            sem.at[t, k],
        )

    def load_rows():
        return pltpu.make_async_copy(rows_vmem, rows_ref, row_sem)

    def unload(t, p, h):
        slot = (2 * t + p) % 2
        columns = pl.ds(t % each * EMB, EMB)
        return pltpu.make_async_copy(
            stage_ref.at[slot, pl.ds(4 * h, 4)],
            outs[4 * (t // each) + 2 * p + h].at[:, :, columns],
            out_sem.at[slot, h],
        )

    def source_of(place):
        outer, inner = place >> 2, place & 3
        step_y = jnp.where(turn < each, outer, inner)
        step_z = jnp.where(turn < each, inner, outer)
        return (((my_y + step_y) & 3) << 2) + ((my_z + step_z) & 3)

    @pl.when((turn == 0) & (part == 0))
    def _():
        for k in range(PIECES):
            load(0, k).start()
        codes = lists_ref[:, 8 * first : 8 * (first + tables), :]
        line = iota(codes.shape, 1)
        rows = (codes & (ROWS_DEV - 1)) + (line >> 3) * ROWS_DEV
        rows_vmem[...] = jnp.where((line & 7) == 4, codes, rows)
        load_rows().start()
        buf_ref[...] = jnp.zeros_like(buf_ref)
        load_rows().wait()

    for t in range(tables):

        @pl.when((turn == t) & (part == 0))
        def _(t=t):
            for k in range(PIECES):
                load(t, k).wait()
            if t + 1 < tables:
                for k in range(PIECES):
                    load(t + 1, k).start()

    def fetch(q, carry):
        source = source_of(part * STEP + q)
        count = rows_ref[source, 8 * turn + 4, 0]
        for line in range(CAP // 128):
            for base in range(0, 128, BLOCK):

                @pl.when(count > line * 128 + base)
                def _(line=line, base=base):
                    for k in range(base, base + BLOCK):
                        ids = rows_ref.at[source, 8 * turn + line, pl.ds(k // 8 * 8, 8)]
                        row = ids[k % 8]
                        buf_ref[q, pl.ds(line * 128 + k, 1), :] = held_ref[pl.ds(row, 1), :]

        return carry

    lax.fori_loop(0, STEP, fetch, 0)
    for t in range(1, tables):
        for p in range(2):

            @pl.when((turn == t) & (part == p))
            def _(t=t, p=p):
                for h in range(2):
                    unload(t - 1, p, h).wait()

    bag = (iota((SAMPLES, 128), 0) + 1).astype(jnp.float32).astype(jnp.bfloat16)
    for q in range(STEP):
        source = source_of(part * STEP + q)
        picks = []
        for line in range(CAP // 128):
            named = lists_ref[source, pl.ds(8 * first + 8 * turn + line, 1), :] >> BAG_SHIFT
            named = named.astype(jnp.float32).astype(jnp.bfloat16)
            picks.append(jnp.where(named == bag, jnp.bfloat16(1), jnp.bfloat16(0)))
        stage_ref[part, q] = jnp.dot(
            jnp.concatenate(picks, axis=1),
            buf_ref[q].astype(jnp.bfloat16),
            preferred_element_type=jnp.float32,
        ).astype(stage_ref.dtype)
    for t in range(tables):
        for p in range(2):

            @pl.when((turn == t) & (part == p))
            def _(t=t, p=p):
                for h in range(2):
                    unload(t, p, h).start()
                if t == tables - 1 and p == 1:
                    for h in range(2):
                        unload(t, 0, h).wait()
                    for h in range(2):
                        unload(t, 1, h).wait()


def pool_tables(first, each, me, lists, table):
    tables = 2 * each
    vmem = pl.BlockSpec(memory_space=pltpu.VMEM)
    hbm = pl.BlockSpec(memory_space=pltpu.HBM)
    return pl.pallas_call(
        functools.partial(pool_kernel, first, each),
        grid=(tables, OWNERS // STEP),
        in_specs=[pl.BlockSpec(memory_space=pltpu.SMEM), vmem, hbm],
        out_specs=[hbm] * 8,
        scratch_shapes=[
            pltpu.VMEM((STEP, CAP, EMB), jnp.float32),
            pltpu.VMEM((2, STEP, SAMPLES, EMB), jnp.bfloat16),
            pltpu.VMEM((tables * ROWS_DEV, EMB), jnp.float32),
            pltpu.VMEM((OWNERS, 8 * tables, 128), jnp.int32),
            pltpu.SMEM((OWNERS, 8 * tables, 128), jnp.int32),
            pltpu.SemaphoreType.DMA((tables, PIECES)),
            pltpu.SemaphoreType.DMA(()),
            pltpu.SemaphoreType.DMA((2, 2)),
        ],
        out_shape=[jax.ShapeDtypeStruct((4, SAMPLES, each * EMB), jnp.bfloat16)] * 8,
        compiler_params=pltpu.CompilerParams(vmem_limit_bytes=48 << 20),
        cost_estimate=pl.CostEstimate(
            flops=10_000_000_000 * tables, transcendentals=0, bytes_accessed=6_000_000
        ),
    )(me, lists, table)


def add_first_kernel(*refs):
    chunks = len(refs) // 8 - 1
    outs = refs[8 * chunks :]
    for half in range(2):
        for k in range(4):
            for c in range(chunks):
                ins = refs[8 * c + 4 * half : 8 * c + 4 * half + 4]
                total = ins[0][k].astype(jnp.float32)
                for d in range(1, 4):
                    total += ins[d][k].astype(jnp.float32)
                outs[4 * half + k][:, c * EMB : (c + 1) * EMB] = total.astype(jnp.bfloat16)


def add_first(parts):
    vmem = pl.BlockSpec(memory_space=pltpu.VMEM)
    width = len(parts) // 8 * EMB
    return pl.pallas_call(
        add_first_kernel,
        in_specs=[vmem] * len(parts),
        out_specs=[vmem] * 8,
        out_shape=[jax.ShapeDtypeStruct((SAMPLES, width), jnp.bfloat16)] * 8,
        compiler_params=pltpu.CompilerParams(vmem_limit_bytes=20 << 20),
        name="add_first",
    )(*parts)


def add_second_kernel(*refs):
    ins, out_ref = refs[:8], refs[8]
    for half in range(2):
        total = ins[4 * half][...].astype(jnp.float32)
        for d in range(1, 4):
            total += ins[4 * half + d][...].astype(jnp.float32)
        total = total.astype(jnp.bfloat16)
        for c in range(total.shape[1] // EMB):
            table = 2 * c + half
            out_ref[:, table * EMB : (table + 1) * EMB] = total[:, c * EMB : (c + 1) * EMB]


def add_second(parts):
    vmem = pl.BlockSpec(memory_space=pltpu.VMEM)
    rows, width = parts[0].shape
    return pl.pallas_call(
        add_second_kernel,
        in_specs=[vmem] * 8,
        out_specs=vmem,
        out_shape=jax.ShapeDtypeStruct((rows, 2 * width), jnp.bfloat16),
        compiler_params=pltpu.CompilerParams(vmem_limit_bytes=16 << 20),
        name="add_second",
    )(*parts)


def score_kernel(pieces, chunks, *refs):
    features = refs[:chunks]
    biases = refs[chunks : chunks + pieces]
    w_in = refs[chunks + pieces : chunks + 2 * pieces]
    w_out = refs[chunks + 2 * pieces : chunks + 3 * pieces]
    out_ref, in_buf, out_buf, in_sem, out_sem = refs[chunks + 3 * pieces :]
    copies = []
    for p in range(pieces):
        first = pltpu.make_async_copy(w_in[p], in_buf.at[p], in_sem.at[p])
        second = pltpu.make_async_copy(w_out[p], out_buf.at[p], out_sem.at[p])
        first.start()
        second.start()
        copies.append((first, second))
    total = None
    for p in range(pieces):
        copies[p][0].wait()
        pre = biases[p][...]
        base = 0
        for feature in features:
            width = feature.shape[1]
            pre = pre + jnp.dot(
                feature[...],
                in_buf[p, base : base + width, :],
                preferred_element_type=jnp.float32,
            )
            base += width
        hidden = jnp.maximum(pre, 0.0).astype(jnp.bfloat16)
        copies[p][1].wait()
        part = jnp.dot(hidden, out_buf[p], preferred_element_type=jnp.float32)
        total = part if total is None else total + part
    out_ref[...] = total.astype(out_ref.dtype)


def score(features, biases, w_in, w_out, dtype):
    pieces, chunks = len(w_in), len(features)
    vmem = pl.BlockSpec(memory_space=pltpu.VMEM)
    hbm = pl.BlockSpec(memory_space=pltpu.HBM)
    return pl.pallas_call(
        functools.partial(score_kernel, pieces, chunks),
        in_specs=[vmem] * (chunks + pieces) + [hbm] * (2 * pieces),
        out_specs=vmem,
        scratch_shapes=[
            pltpu.VMEM((pieces, *w_in[0].shape), jnp.bfloat16),
            pltpu.VMEM((pieces, *w_out[0].shape), jnp.bfloat16),
            pltpu.SemaphoreType.DMA((pieces,)),
            pltpu.SemaphoreType.DMA((pieces,)),
        ],
        out_shape=jax.ShapeDtypeStruct((SAMPLES, w_out[0].shape[1]), dtype),
        compiler_params=pltpu.CompilerParams(vmem_limit_bytes=40 << 20),
        cost_estimate=pl.CostEstimate(
            flops=10_000_000_000, transcendentals=0, bytes_accessed=14_000_000
        ),
    )(*features, *biases, *w_in, *w_out)


def to_chip(array, targets):
    return lax.ppermute(
        array, "gy", [(x * 2 + c, targets[c](x) * 2 + c) for x in range(4) for c in range(2)]
    )


def flip(x):
    return x ^ 1


def mirror(x):
    return 3 - x


def along(array, axis, shift):
    if axis == "y":
        pairs = [(y * 4 + z, (y + shift) % 4 * 4 + z) for y in range(4) for z in range(4)]
    else:
        pairs = [(y * 4 + z, y * 4 + (z + shift) % 4) for y in range(4) for z in range(4)]
    return lax.ppermute(array, "gx", pairs)


def moved(parts, axes):
    out = list(parts)
    for shift in (2, 1, 3):
        for half in range(2):
            out[4 * half + shift] = along(parts[4 * half + shift], axes[half], shift)
    return out


def to_core(array):
    return lax.ppermute(array, "gy", [(k, k ^ 1) for k in range(8)])


def local(table, lookup_owner, lookup_row, bag_length, top_in, top_bias, top_out):
    own = (top_bias.reshape(1, -1), top_in, top_out)
    near, far, far_near = [], [], []
    for k, array in enumerate(own):
        near.append(to_core(array))
        far.append(to_chip(array, (mirror, flip)))
        far_near.append(to_chip(near[k], (mirror, flip)))
    biases, w_in, w_out = zip(own, near, far, far_near)

    owner = jnp.transpose(lookup_owner, (0, 2, 3, 1))
    row = jnp.transpose(lookup_row, (0, 2, 1))
    lists = pl.pallas_call(
        dispatch_kernel,
        out_shape=jax.ShapeDtypeStruct((OWNERS, 8 * TABLES, 128), jnp.int32),
        name="dispatch",
    )(owner, row, bag_length)
    lists = lax.all_to_all(lists, "gx", 0, 0, tiled=True)

    me = lax.axis_index("gx").astype(jnp.int32).reshape(1)
    parts = []
    for first in range(0, TABLES, 2):
        shares = pool_tables(first, 1, me, lists, table)
        parts += moved(shares, "yz")
    parts = moved(add_first(parts), "zy")
    mine = add_second(parts)
    theirs = to_chip(mine, (flip, mirror))
    kept = score([mine], biases, w_in, w_out, jnp.float32)
    sent = score([theirs], biases, w_in, w_out, jnp.bfloat16)
    received = to_chip(sent, (flip, mirror))
    return (kept + received.astype(jnp.float32)).astype(jnp.bfloat16)


def solution(mesh):
    return jax.shard_map(
        local,
        mesh=mesh,
        in_specs=(
            P(None, "gx", None),
            P(None, ("gx", "gy"), None, None),
            P(None, ("gx", "gy"), None),
            P(None, ("gx", "gy")),
            P(None, "gy"),
            P("gy"),
            P("gy", None),
        ),
        out_specs=P(("gx", "gy"), None),
        check_vma=False,
    )
```

```python
import functools

import jax
import jax.numpy as jnp
from jax import lax
from jax.experimental import pallas as pl
from jax.experimental.pallas import tpu as pltpu
from jax.sharding import PartitionSpec as P


TABLES = 4
SAMPLES = 256
BAG = 16
OWNERS = 16
CAP = 512
ROWS_DEV = 8192
EMB = 128
BLOCK = 64
PIECES = 4
STEP = 8
BAG_SHIFT = 13


def iota(shape, dim):
    return lax.broadcasted_iota(jnp.int32, shape, dim)


def ones_where(mask):
    return jnp.where(mask, 1.0, 0.0).astype(jnp.bfloat16)


def dispatch_kernel(own_ref, row_ref, length_ref, out_ref):
    before = ones_where(iota((256, 256), 0) < iota((256, 256), 1))
    r, c = iota((256, 256), 0), iota((256, 256), 1)
    earlier = ones_where(((r & 15) == (c & 15)) & ((c >> 4) < (r >> 4)))
    ones = jnp.ones((256, 256), jnp.bfloat16)
    same = ones_where(iota((16, 256), 0) == (iota((16, 256), 1) & 15))
    owner_iota = iota((16, 16, 256), 1)
    count64 = iota((64, 256), 0).astype(jnp.float32).astype(jnp.bfloat16)
    count128 = iota((128, 256), 0).astype(jnp.float32).astype(jnp.bfloat16)
    bag = (iota((1, 256), 1) + 1).astype(jnp.float32).astype(jnp.bfloat16)
    zero, one = jnp.bfloat16(0), jnp.bfloat16(1)
    for t in range(TABLES):
        live = iota((BAG, SAMPLES), 0) < length_ref[t : t + 1, :]
        own = jnp.where(live, own_ref[t, :, 0, :], OWNERS)
        mark = (own[:, None, :] == owner_iota).reshape(256, 256)
        onehot = ones_where(mark)
        rank = jnp.dot(onehot, before, preferred_element_type=jnp.float32)
        lead = jnp.dot(earlier, onehot, preferred_element_type=jnp.float32)
        rank += jnp.dot(lead.astype(jnp.bfloat16), ones, preferred_element_type=jnp.float32)
        rank = jnp.sum(jnp.where(mark, rank, 0.0).reshape(16, 16, 256), axis=1).astype(jnp.int32)
        total = jnp.dot(same, onehot, preferred_element_type=jnp.float32)
        total = jnp.dot(total.astype(jnp.bfloat16), ones, preferred_element_type=jnp.float32)
        hi = (own * 4 + (rank >> 7)).astype(jnp.float32)
        lo = (rank & 127).astype(jnp.float32)
        row = row_ref[t]
        low = (row & 255).astype(jnp.float32)
        high = (row >> 8).astype(jnp.float32)
        acc = jnp.zeros((192, 128), jnp.float32)
        for s in range(BAG):
            line = slice(s, s + 1)
            left = hi[line].astype(jnp.bfloat16) == count64
            planes = jnp.concatenate(
                [
                    jnp.where(left, low[line].astype(jnp.bfloat16), zero),
                    jnp.where(left, high[line].astype(jnp.bfloat16), zero),
                    jnp.where(left, bag, zero),
                ],
                axis=0,
            )
            right = jnp.where(lo[line].astype(jnp.bfloat16) == count128, one, zero)
            acc += lax.dot_general(
                planes, right, (((1,), (1,)), ((), ())), preferred_element_type=jnp.float32
            )
        acc = acc.astype(jnp.int32)
        code = acc[:64] | (acc[64:128] << 8) | (acc[128:] << BAG_SHIFT)
        out_ref[:, 8 * t : 8 * t + 4, :] = code.reshape(OWNERS, 4, 128)
        out_ref[:, 8 * t + 4, :] = total[:, :128].astype(jnp.int32)
        out_ref[:, 8 * t + 5 : 8 * t + 8, :] = jnp.zeros((OWNERS, 3, 128), jnp.int32)


def pool_kernel(first, ready, ahead, me_ref, lists_ref, table_ref, *refs):
    each, tables = 1, 2
    here_ref, refs = (refs[0], refs[1:]) if ready else (None, refs)
    outs, refs = refs[:8], refs[8:]
    next_ref, refs = (refs[0], refs[1:]) if ahead else (None, refs)
    buf_ref, stage_ref, held_ref, rows_vmem, rows_ref, sem, row_sem, out_sem = refs[:8]
    skip = int(ready)
    turn, part = pl.program_id(0), pl.program_id(1)
    my_y, my_z = me_ref[0] >> 2, me_ref[0] & 3

    def load(t, k):
        size = ROWS_DEV // PIECES
        return pltpu.make_async_copy(
            table_ref.at[first + t, pl.ds(k * size, size)],
            held_ref.at[pl.ds((t - skip) * ROWS_DEV + k * size, size)],
            sem.at[t, k],
        )

    def load_next():
        return pltpu.make_async_copy(table_ref.at[first + tables], next_ref, refs[8])

    def load_rows(place):
        source = source_of(place)
        return pltpu.make_async_copy(
            rows_vmem.at[source], rows_ref.at[source], row_sem.at[place]
        )

    def unload(t, p, h):
        slot = (2 * t + p) % 2
        columns = pl.ds(t % each * EMB, EMB)
        return pltpu.make_async_copy(
            stage_ref.at[slot, pl.ds(4 * h, 4)],
            outs[4 * (t // each) + 2 * p + h].at[:, :, columns],
            out_sem.at[slot, h],
        )

    def source_of(place):
        outer, inner = place >> 2, place & 3
        step_y = jnp.where(turn < each, outer, inner)
        step_z = jnp.where(turn < each, inner, outer)
        return (((my_y + step_y) & 3) << 2) + ((my_z + step_z) & 3)

    @pl.when((turn == 0) & (part == 0))
    def _():
        for k in range(PIECES):
            load(skip, k).start()
        codes = lists_ref[:, 8 * first : 8 * (first + tables), :]
        line = iota(codes.shape, 1)
        rows = (codes & (ROWS_DEV - 1)) + ((line >> 3) - skip) * ROWS_DEV * (1 - skip)
        rows_vmem[...] = jnp.where((line & 7) == 4, codes, rows)
        for place in range(OWNERS):
            load_rows(place).start()
        buf_ref[...] = jnp.zeros_like(buf_ref)

    for t in range(tables):

        @pl.when((turn == t) & (part == 0))
        def _(t=t):
            if t >= skip:
                for k in range(PIECES):
                    load(t, k).wait()
            if skip <= t < tables - 1:
                for k in range(PIECES):
                    load(t + 1, k).start()
            if ahead and t == tables - 1:
                load_next().start()

    def fetch(source_ref, q, carry):
        source = source_of(part * STEP + q)

        @pl.when(turn == 0)
        def _():
            load_rows(part * STEP + q).wait()

        count = rows_ref[source, 8 * turn + 4, 0]
        for line in range(CAP // 128):
            for base in range(0, 128, BLOCK):

                @pl.when(count > line * 128 + base)
                def _(line=line, base=base):
                    for k in range(base, base + BLOCK):
                        ids = rows_ref.at[source, 8 * turn + line, pl.ds(k // 8 * 8, 8)]
                        row = ids[k % 8]
                        buf_ref[q, pl.ds(line * 128 + k, 1), :] = source_ref[pl.ds(row, 1), :]

        return carry

    if ready:

        @pl.when(turn == 0)
        def _():
            lax.fori_loop(0, STEP, functools.partial(fetch, here_ref), 0)

        @pl.when(turn > 0)
        def _():
            lax.fori_loop(0, STEP, functools.partial(fetch, held_ref), 0)

    else:
        lax.fori_loop(0, STEP, functools.partial(fetch, held_ref), 0)
    for t in range(1, tables):
        for p in range(2):

            @pl.when((turn == t) & (part == p))
            def _(t=t, p=p):
                for h in range(2):
                    unload(t - 1, p, h).wait()

    bag = (iota((SAMPLES, 128), 0) + 1).astype(jnp.float32).astype(jnp.bfloat16)
    for q in range(STEP):
        source = source_of(part * STEP + q)
        picks = []
        for line in range(CAP // 128):
            named = lists_ref[source, pl.ds(8 * first + 8 * turn + line, 1), :] >> BAG_SHIFT
            named = named.astype(jnp.float32).astype(jnp.bfloat16)
            picks.append(jnp.where(named == bag, jnp.bfloat16(1), jnp.bfloat16(0)))
        stage_ref[part, q] = jnp.dot(
            jnp.concatenate(picks, axis=1),
            buf_ref[q].astype(jnp.bfloat16),
            preferred_element_type=jnp.float32,
        ).astype(stage_ref.dtype)
    for t in range(tables):
        for p in range(2):

            @pl.when((turn == t) & (part == p))
            def _(t=t, p=p):
                for h in range(2):
                    unload(t, p, h).start()
                if t == tables - 1 and p == 1:
                    for h in range(2):
                        unload(t, 0, h).wait()
                    for h in range(2):
                        unload(t, 1, h).wait()
                    if ahead:
                        load_next().wait()


def pool_tables(first, me, lists, table, here=None, ahead=False):
    tables, ready = 2, here is not None
    vmem = pl.BlockSpec(memory_space=pltpu.VMEM)
    hbm = pl.BlockSpec(memory_space=pltpu.HBM)
    return pl.pallas_call(
        functools.partial(pool_kernel, first, ready, ahead),
        grid=(tables, OWNERS // STEP),
        in_specs=[pl.BlockSpec(memory_space=pltpu.SMEM), vmem, hbm] + [vmem] * ready,
        out_specs=[hbm] * 8 + [vmem] * ahead,
        scratch_shapes=[
            pltpu.VMEM((STEP, CAP, EMB), jnp.float32),
            pltpu.VMEM((2, STEP, SAMPLES, EMB), jnp.bfloat16),
            pltpu.VMEM(((tables - ready) * ROWS_DEV, EMB), jnp.float32),
            pltpu.VMEM((OWNERS, 8 * tables, 128), jnp.int32),
            pltpu.SMEM((OWNERS, 8 * tables, 128), jnp.int32),
            pltpu.SemaphoreType.DMA((tables, PIECES)),
            pltpu.SemaphoreType.DMA((OWNERS,)),
            pltpu.SemaphoreType.DMA((2, 2)),
        ]
        + [pltpu.SemaphoreType.DMA(())] * ahead,
        out_shape=[jax.ShapeDtypeStruct((4, SAMPLES, EMB), jnp.bfloat16)] * 8
        + [jax.ShapeDtypeStruct((ROWS_DEV, EMB), jnp.float32)] * ahead,
        compiler_params=pltpu.CompilerParams(vmem_limit_bytes=40 << 20),
        cost_estimate=pl.CostEstimate(
            flops=10_000_000_000 * tables, transcendentals=0, bytes_accessed=6_000_000
        ),
    )(me, lists, table, *([here] if ready else []))


def add_first_kernel(*refs):
    chunks = len(refs) // 8 - 1
    outs = refs[8 * chunks :]
    for half in range(2):
        for k in range(4):
            for c in range(chunks):
                ins = refs[8 * c + 4 * half : 8 * c + 4 * half + 4]
                total = ins[0][k].astype(jnp.float32)
                for d in range(1, 4):
                    total += ins[d][k].astype(jnp.float32)
                outs[4 * half + k][:, c * EMB : (c + 1) * EMB] = total.astype(jnp.bfloat16)


def add_first(parts):
    vmem = pl.BlockSpec(memory_space=pltpu.VMEM)
    width = len(parts) // 8 * EMB
    return pl.pallas_call(
        add_first_kernel,
        in_specs=[vmem] * len(parts),
        out_specs=[vmem] * 8,
        out_shape=[jax.ShapeDtypeStruct((SAMPLES, width), jnp.bfloat16)] * 8,
        compiler_params=pltpu.CompilerParams(vmem_limit_bytes=20 << 20),
        name="add_first",
    )(*parts)


def add_second_kernel(*refs):
    ins, out_ref = refs[:8], refs[8]
    for half in range(2):
        total = ins[4 * half][...].astype(jnp.float32)
        for d in range(1, 4):
            total += ins[4 * half + d][...].astype(jnp.float32)
        total = total.astype(jnp.bfloat16)
        for c in range(total.shape[1] // EMB):
            table = 2 * c + half
            out_ref[:, table * EMB : (table + 1) * EMB] = total[:, c * EMB : (c + 1) * EMB]


def add_second(parts):
    vmem = pl.BlockSpec(memory_space=pltpu.VMEM)
    rows, width = parts[0].shape
    return pl.pallas_call(
        add_second_kernel,
        in_specs=[vmem] * 8,
        out_specs=vmem,
        out_shape=jax.ShapeDtypeStruct((rows, 2 * width), jnp.bfloat16),
        compiler_params=pltpu.CompilerParams(vmem_limit_bytes=16 << 20),
        name="add_second",
    )(*parts)


def score_kernel(pieces, chunks, *refs):
    features = refs[:chunks]
    biases = refs[chunks : chunks + pieces]
    w_in = refs[chunks + pieces : chunks + 2 * pieces]
    w_out = refs[chunks + 2 * pieces : chunks + 3 * pieces]
    out_ref, in_buf, out_buf, in_sem, out_sem = refs[chunks + 3 * pieces :]
    copies = []
    for p in range(pieces):
        first = pltpu.make_async_copy(w_in[p], in_buf.at[p], in_sem.at[p])
        second = pltpu.make_async_copy(w_out[p], out_buf.at[p], out_sem.at[p])
        first.start()
        second.start()
        copies.append((first, second))
    total = None
    for p in range(pieces):
        copies[p][0].wait()
        pre = biases[p][...]
        base = 0
        for feature in features:
            width = feature.shape[1]
            pre = pre + jnp.dot(
                feature[...],
                in_buf[p, base : base + width, :],
                preferred_element_type=jnp.float32,
            )
            base += width
        hidden = jnp.maximum(pre, 0.0).astype(jnp.bfloat16)
        copies[p][1].wait()
        part = jnp.dot(hidden, out_buf[p], preferred_element_type=jnp.float32)
        total = part if total is None else total + part
    out_ref[...] = total.astype(out_ref.dtype)


def score(features, biases, w_in, w_out, dtype):
    pieces, chunks = len(w_in), len(features)
    vmem = pl.BlockSpec(memory_space=pltpu.VMEM)
    hbm = pl.BlockSpec(memory_space=pltpu.HBM)
    return pl.pallas_call(
        functools.partial(score_kernel, pieces, chunks),
        in_specs=[vmem] * (chunks + pieces) + [hbm] * (2 * pieces),
        out_specs=vmem,
        scratch_shapes=[
            pltpu.VMEM((pieces, *w_in[0].shape), jnp.bfloat16),
            pltpu.VMEM((pieces, *w_out[0].shape), jnp.bfloat16),
            pltpu.SemaphoreType.DMA((pieces,)),
            pltpu.SemaphoreType.DMA((pieces,)),
        ],
        out_shape=jax.ShapeDtypeStruct((SAMPLES, w_out[0].shape[1]), dtype),
        compiler_params=pltpu.CompilerParams(vmem_limit_bytes=40 << 20),
        cost_estimate=pl.CostEstimate(
            flops=10_000_000_000, transcendentals=0, bytes_accessed=14_000_000
        ),
    )(*features, *biases, *w_in, *w_out)


def to_chip(array, targets):
    return lax.ppermute(
        array, "gy", [(x * 2 + c, targets[c](x) * 2 + c) for x in range(4) for c in range(2)]
    )


def flip(x):
    return x ^ 1


def mirror(x):
    return 3 - x


def along(array, axis, shift):
    if axis == "y":
        pairs = [(y * 4 + z, (y + shift) % 4 * 4 + z) for y in range(4) for z in range(4)]
    else:
        pairs = [(y * 4 + z, y * 4 + (z + shift) % 4) for y in range(4) for z in range(4)]
    return lax.ppermute(array, "gx", pairs)


def moved(parts, axes):
    out = list(parts)
    for shift in (2, 1, 3):
        for half in range(2):
            out[4 * half + shift] = along(parts[4 * half + shift], axes[half], shift)
    return out


def to_core(array):
    return lax.ppermute(array, "gy", [(k, k ^ 1) for k in range(8)])


def local(table, lookup_owner, lookup_row, bag_length, top_in, top_bias, top_out):
    own = (top_bias.reshape(1, -1), top_in, top_out)
    near, far, far_near = [], [], []
    for k, array in enumerate(own):
        near.append(to_core(array))
        far.append(to_chip(array, (mirror, flip)))
        far_near.append(to_chip(near[k], (mirror, flip)))
    biases, w_in, w_out = zip(own, near, far, far_near)

    owner = jnp.transpose(lookup_owner, (0, 2, 3, 1))
    row = jnp.transpose(lookup_row, (0, 2, 1))
    lists = pl.pallas_call(
        dispatch_kernel,
        out_shape=jax.ShapeDtypeStruct((OWNERS, 8 * TABLES, 128), jnp.int32),
        name="dispatch",
    )(owner, row, bag_length)
    lists = lax.all_to_all(lists, "gx", 0, 0, tiled=True)

    me = lax.axis_index("gx").astype(jnp.int32).reshape(1)
    parts, here = [], None
    for first in range(0, TABLES, 2):
        shares = pool_tables(first, me, lists, table, here, first == 0)
        here = shares[8] if first == 0 else None
        parts += moved(shares[:8], "yz")
    parts = add_first(parts)
    parts = moved(parts, "zy")
    mine = add_second(parts)
    theirs = to_chip(mine, (flip, mirror))
    kept = score([mine], biases, w_in, w_out, jnp.float32)
    sent = score([theirs], biases, w_in, w_out, jnp.bfloat16)
    received = to_chip(sent, (flip, mirror))
    return (kept + received.astype(jnp.float32)).astype(jnp.bfloat16)


def solution(mesh):
    return jax.shard_map(
        local,
        mesh=mesh,
        in_specs=(
            P(None, "gx", None),
            P(None, ("gx", "gy"), None, None),
            P(None, ("gx", "gy"), None),
            P(None, ("gx", "gy")),
            P(None, "gy"),
            P("gy"),
            P("gy", None),
        ),
        out_specs=P(("gx", "gy"), None),
        check_vma=False,
    )
```
